256 devices in a mesh: gx: 16 (over z, x_lo), gy: 16 (over y, x_hi, core).
Axes of the slice: x: 4 (x_hi: 2, x_lo: 2; x = x_hi * 2 + x_lo), y: 4, z: 8, core: 2. Of those that a mesh axis runs over, the one named last changes fastest.
Arguments:
- gradient: float32 [2048, 512], P('gx', 'gy'), may hold values from -6 to 6
- stat_old: float32 [2048, 2048], P('gx', 'gy'), may hold values from -1.001 to 1.001, as said below
Outputs:
- statistic: float32 [2048, 2048], P('gx', 'gy')
- inverse_root: float32 [2048, 2048], P('gx', 'gy')
The draws below stay inside these ranges and needn't reach their ends.
Inputs may be any that keep to these rules, and one draw needn't show every extreme that they name: stat_old is symmetric positive semidefinite with unit diagonal, the Gram matrix of 2048 unit-length rows of 512 entries.
All inputs are finite; a program needn't handle non-finite values.
Results may differ from the reference program's by a relative error of at most 0.0003.
Values sent between devices are 32-bit elements.
A program may use at most 64 MiB of HBM per device.

```python
import jax
import jax.numpy as jnp
from jax import lax

NSIDE = 2048
MCOLS = 512


def draw_stat_old(key, part):
    factor = jax.random.normal(key, (NSIDE, NSIDE // 4), jnp.float32)
    lengths = jnp.sqrt(jnp.sum(factor * factor, axis=1, keepdims=True))
    factor = factor / lengths
    return jnp.dot(factor, factor.T, preferred_element_type=jnp.float32, precision=lax.Precision.HIGHEST)


def steps_of(stream_key, dims, pieces, low, high):
    factor_of = 1.0
    for dim, shards_of in pieces:
        draws = jax.random.uniform(jax.random.fold_in(jax.random.fold_in(stream_key, 6), dim), (shards_of,), jnp.float32, low / len(pieces), high / len(pieces))
        factor_of = factor_of * jnp.repeat(jnp.exp(draws), dims[dim] // shards_of).reshape((-1,) + (1,) * (len(dims) - 1 - dim))
    return factor_of


def bell_draw(rng, dims, width, reach, pieces=(), kind=jnp.bfloat16):
    array = jax.random.normal(rng, dims, jnp.float32) * width
    if len(pieces) > 0:
        array = steps_of(rng, dims, pieces, -0.22, 0.18) * array
    return jnp.clip(array, min=-reach, max=reach).astype(kind)


def setup_inputs(seed: int = 0) -> dict:
    key_of = jax.random.split(jax.random.key(seed), 3)
    return {
        "gradient": bell_draw(key_of[0], (NSIDE, MCOLS), 1.0, 6.0, ((0, 16), (1, 16)), jnp.float32),
        "stat_old": draw_stat_old(jax.random.fold_in(key_of[2], 71), 0),
    }


def matmul(leading, trailing):
    return jnp.dot(leading, trailing, preferred_element_type=jnp.float32, precision=lax.Precision.HIGHEST)

def reference(gradient, stat_old):
    statistic = 0.9 * stat_old + matmul(gradient, gradient.T) / MCOLS
    divisor = 2.0 * jnp.sqrt(jnp.sum(statistic * statistic) / NSIDE)
    identity = jnp.eye(NSIDE, dtype=jnp.float32)
    normed = statistic / divisor
    first_step = 1.5 * identity - 0.5 * normed
    root_half = matmul(normed, first_step)
    product_mid = matmul(first_step, root_half)
    second_step = 1.5 * identity - 0.5 * product_mid
    inverse_root = matmul(second_step, first_step)
    return (statistic, inverse_root)
```

```python
import functools

import jax
import jax.numpy as jnp
from jax import lax
from jax.experimental import pallas as pl
from jax.experimental.pallas import tpu as pltpu
from jax.sharding import Mesh
from jax.sharding import PartitionSpec as P

MESH = pl.DeviceIdType.MESH
GX = ("z", "a")
GY = ("y", "b", "c")
B = 128
HALF = 64
PAD = 8
KP = 32
N = 16

A0, A1, A2, A3, A4 = 2.25, -2.4375, 1.6875, -0.5625, 0.0625


def split(x):
    hi = x.astype(jnp.bfloat16)
    lo = (x - hi.astype(jnp.float32)).astype(jnp.bfloat16)
    return hi, lo


def fold4(full):
    return (full[:B, :B] + full[B:, :B]) + (full[:B, B:] + full[B:, B:])


def kernel(
    g_hbm, a_hbm, s_out, r_out,
    a_in, gt, GI, GJ, R1, C1, R2, C2,
    in_sem, gi_sem, gj_sem, gs_sem, r1_sem, c1_sem, r2_sem, c2_sem, send_sem,
):
    z, a = lax.axis_index("z"), lax.axis_index("a")
    y, b, c = lax.axis_index("y"), lax.axis_index("b"), lax.axis_index("c")
    gi = z * 2 + a
    gj = y * 4 + b * 2 + c
    a1, b1, c1 = 1 - a, 1 - b, 1 - c
    off_diag = gi != gj

    load_g = pltpu.make_async_copy(g_hbm, gt, in_sem.at[0])
    load_a = pltpu.make_async_copy(a_hbm, a_in, in_sem.at[1])
    load_g.start()
    load_a.start()

    def gx_of(s):
        i = lax.rem(gi + s, N)
        return i // 2, lax.rem(i, 2)

    def gy_of(j):
        return j // 4, lax.rem(j // 2, 2), lax.rem(j, 2)

    barrier = pltpu.get_barrier_semaphore()

    def greet(**where):
        pl.semaphore_signal(barrier, inc=1, device_id=where, device_id_type=MESH)

    zj, aj = gj // 2, lax.rem(gj, 2)

    @pl.when(off_diag)
    def _():
        for k in range(N):
            greet(z=zj, a=aj, y=k // 4, b=(k // 2) % 2, c=k % 2)

    for s in range(1, N):
        py, pb, pc = gy_of(lax.rem(gj + s, N))
        greet(y=py, b=pb, c=pc)
    up, down = lax.rem(z + 1, 8), lax.rem(z + 7, 8)
    greet(z=up)
    greet(z=down)
    greet(a=a1)

    load_g.wait()
    GI[gj] = gt[...]
    pl.semaphore_wait(barrier, 33)

    sends = []

    def send(src, dst, rsem, **where):
        copy = pltpu.make_async_remote_copy(
            src_ref=src, dst_ref=dst, send_sem=send_sem.at[len(sends)], recv_sem=rsem,
            device_id=where, device_id_type=MESH,
        )
        copy.start()
        sends.append(copy)

    def arrived(ref, rsem):
        pltpu.make_async_remote_copy(
            src_ref=ref, dst_ref=ref, send_sem=gs_sem, recv_sem=rsem,
            device_id={"a": a1}, device_id_type=MESH,
        ).wait_recv()

    iy, ib, ic = gy_of(gi)
    for s in (8, 7, 9, 6, 10, 5, 11, 4, 12, 3, 13, 2, 14, 1, 15):
        pz, pa = gx_of(s)
        send(gt, GJ.at[gj], gj_sem.at[gj], z=pz, a=pa, y=iy, b=ib, c=ic)
    for s in (8, 7, 9, 6, 10, 5, 11, 4, 12, 3, 13, 2, 14, 1, 15):
        py, pb, pc = gy_of(lax.rem(gj + s, N))
        send(gt, GI.at[gj], gi_sem.at[gj], y=py, b=pb, c=pc)

    for s in range(1, N):
        k = lax.rem(gj + s, N)
        arrived(GI.at[k], gi_sem.at[k])

    @pl.when(off_diag)
    def _():
        for k in range(N):
            arrived(GJ.at[k], gj_sem.at[k])

    @pl.when(jnp.logical_not(off_diag))
    def _():
        GJ[...] = GI[...]

    load_a.wait()
    left = jnp.transpose(GI[...].reshape(N * KP, B))
    right = GJ[...].reshape(N * KP, B)
    lh, ll = split(left)
    rh, rl = split(right)
    full = jnp.dot(
        jnp.concatenate([lh, ll], axis=0), jnp.concatenate([rh, rl], axis=1),
        preferred_element_type=jnp.float32,
    )
    stat = 0.9 * a_in[...] + fold4(full) / float(N * KP)
    s_out[...] = stat
    R1[gj] = stat
    C1[gi] = stat

    def exchange(R, C, rsem, csem, rows):
        parts = ((0, HALF), (HALF, rows - HALF))

        def row_ref(dy, bb, cc):
            k = lax.rem(y + dy, 4) * 4 + bb * 2 + cc
            return R.at[k], rsem.at[k]

        def col_ref(dz, aa, h):
            k = lax.rem(z + dz + 8, 8) * 2 + aa
            return C.at[k, pl.ds(*parts[h])], csem.at[k, h]

        def fwd(item, **where):
            ref, sem = item
            send(ref, ref, sem, **where)

        def got(item):
            arrived(*item)

        mine = row_ref(0, b, c)
        for h in (0, 1):
            fwd(col_ref(0, a, h), z=up)
            fwd(col_ref(0, a, h), z=down)
            fwd(col_ref(0, a, h), a=a1)
        fwd(mine, b=b1)
        fwd(mine, y=lax.rem(y + 1, 4))
        fwd(mine, y=lax.rem(y + 3, 4))
        fwd(mine, y=lax.rem(y + 2, 4))
        fwd(mine, c=c1)

        for h in (0, 1):
            got(col_ref(-1, a, h))
            fwd(col_ref(-1, a, h), z=up)
            got(col_ref(1, a, h))
            fwd(col_ref(1, a, h), z=down)
            got(col_ref(0, a1, h))
            fwd(col_ref(0, a1, h), z=up)
            fwd(col_ref(0, a1, h), z=down)
        for dy in (1, 3):
            got(row_ref(dy, b, c))
            fwd(row_ref(dy, b, c), c=c1)
        got(row_ref(0, b1, c))
        fwd(row_ref(0, b1, c), y=lax.rem(y + 1, 4))
        fwd(row_ref(0, b1, c), y=lax.rem(y + 3, 4))
        fwd(row_ref(0, b1, c), y=lax.rem(y + 2, 4))
        fwd(row_ref(0, b1, c), c=c1)
        for h in (0, 1):
            got(col_ref(-2, a, h))
            fwd(col_ref(-2, a, h), z=up)
            got(col_ref(2, a, h))
            fwd(col_ref(2, a, h), z=down)
            got(col_ref(-1, a1, h))
            fwd(col_ref(-1, a1, h), z=up)
            got(col_ref(1, a1, h))
            fwd(col_ref(1, a1, h), z=down)
        got(row_ref(2, b, c))
        fwd(row_ref(2, b, c), c=c1)
        for h in (0, 1):
            got(col_ref(-3, a, h))
            if h == 0:
                fwd(col_ref(-3, a, h), z=up)
            fwd(col_ref(-3, a, h), a=a1)
            got(col_ref(3, a, h))
            if h == 1:
                fwd(col_ref(3, a, h), z=down)
            fwd(col_ref(3, a, h), a=a1)
        for dy in (1, 3, 2):
            got(row_ref(dy, b1, c))
            fwd(row_ref(dy, b1, c), c=c1)
        for h in (0, 1):
            got(col_ref(4, a, h))
            fwd(col_ref(4, a, h), a=a1)
        for dy, bb in ((0, b), (1, b), (3, b), (0, b1), (2, b), (1, b1), (3, b1), (2, b1)):
            got(row_ref(dy, bb, c1))
        for dz in (-2, 2):
            for h in (0, 1):
                got(col_ref(dz, a1, h))
        for dz in (-3, 3, 4):
            for h in (0, 1):
                got(col_ref(dz, a1, h))

    exchange(R1, C1, r1_sem, c1_sem, B)

    def strips(R, k):
        rows = jnp.concatenate([R[2 * k], R[2 * k + 1]], axis=1)
        hi, lo = split(rows)
        return jnp.concatenate([hi, lo], axis=0)

    def columns(C, k):
        rows = jnp.concatenate([C[2 * k, :B], C[2 * k + 1, :B]], axis=0)
        hi, lo = split(rows)
        return jnp.concatenate([hi, lo], axis=1)

    squares = jnp.zeros((PAD, B), jnp.float32)
    total = jnp.zeros((2 * B, 2 * B), jnp.float32)
    for k in range(8):
        total = total + jnp.dot(strips(R1, k), columns(C1, k), preferred_element_type=jnp.float32)
    for k in range(N):
        block = R1[k]
        squares = squares + jnp.sum((block * block).reshape(B // PAD, PAD, B), axis=0)
    mid = fold4(total)
    R2[gj] = mid
    C2[gi, :B] = mid
    C2[gi, B:] = squares

    exchange(R2, C2, r2_sem, c2_sem, B + PAD)

    wide = jnp.zeros((2 * B, 4 * B), jnp.float32)
    for k in range(8):
        both = jnp.concatenate([columns(C1, k), columns(C2, k)], axis=1)
        wide = wide + jnp.dot(strips(R2, k), both, preferred_element_type=jnp.float32)
    cube = fold4(wide[:, : 2 * B])
    quad = fold4(wide[:, 2 * B:])
    squares = jnp.zeros((PAD, B), jnp.float32)
    for k in range(N):
        squares = squares + C2[k, B:]
    whole = jnp.sum(squares, keepdims=True)
    inv = 1.0 / (2.0 * jnp.sqrt(whole / float(N * B)))
    rows = lax.broadcasted_iota(jnp.int32, (B, B), 0) + gi * B
    cols = lax.broadcasted_iota(jnp.int32, (B, B), 1) + gj * B
    eye = jnp.where(rows == cols, A0, 0.0)
    tail = A2 * R2[gj] + inv * (A3 * cube + inv * (A4 * quad))
    r_out[...] = eye + inv * (A1 * R1[gj] + inv * tail)

    for copy in sends:
        copy.wait_send()


def local(gradient, stat_old):
    f32 = jnp.float32
    dma = pltpu.SemaphoreType.DMA
    return pl.pallas_call(
        kernel,
        out_shape=(jax.ShapeDtypeStruct((B, B), f32), jax.ShapeDtypeStruct((B, B), f32)),
        in_specs=[pl.BlockSpec(memory_space=pl.ANY)] * 2,
        out_specs=[pl.BlockSpec(memory_space=pltpu.VMEM)] * 2,
        scratch_shapes=[
            pltpu.VMEM((B, B), f32),
            pltpu.VMEM((KP, B), f32),
            pltpu.VMEM((N, KP, B), f32),
            pltpu.VMEM((N, KP, B), f32),
            pltpu.VMEM((N, B, B), f32),
            pltpu.VMEM((N, B, B), f32),
            pltpu.VMEM((N, B, B), f32),
            pltpu.VMEM((N, B + PAD, B), f32),
            dma((2,)),
            dma((N,)),
            dma((N,)),
            dma,
            dma((N,)),
            dma((N, 2)),
            dma((N,)),
            dma((N, 2)),
            dma((128,)),
        ],
        compiler_params=pltpu.CompilerParams(collective_id=0, has_side_effects=True),
    )(gradient.T, stat_old)


def solution(mesh):
    torus = Mesh(mesh.devices.reshape(8, 2, 4, 2, 2), ("z", "a", "y", "b", "c"))
    return jax.shard_map(
        local, mesh=torus, in_specs=(P(GX, GY), P(GX, GY)),
        out_specs=(P(GX, GY), P(GX, GY)), check_vma=False,
    )
```

```python
import functools

import jax
import jax.numpy as jnp
from jax import lax
from jax.experimental import pallas as pl
from jax.experimental.pallas import tpu as pltpu
from jax.sharding import Mesh
from jax.sharding import PartitionSpec as P

MESH = pl.DeviceIdType.MESH
GX = ("z", "a")
GY = ("y", "b", "c")
B = 128
CH = 4
PAD = 8
KP = 32
N = 16

A0, A1, A2, A3, A4 = 2.25, -2.4375, 1.6875, -0.5625, 0.0625


def split(x):
    hi = x.astype(jnp.bfloat16)
    lo = (x - hi.astype(jnp.float32)).astype(jnp.bfloat16)
    return hi, lo


def fold4(full):
    return (full[:B, :B] + full[B:, :B]) + (full[:B, B:] + full[B:, B:])


def kernel(
    g_hbm, a_hbm, s_out, r_out,
    a_in, gt, GI, GJ, R1, C1, R2, C2,
    in_sem, gi_sem, gj_sem, gs_sem, r1_sem, c1_sem, r2_sem, c2_sem, send_sem,
):
    z, a = lax.axis_index("z"), lax.axis_index("a")
    y, b, c = lax.axis_index("y"), lax.axis_index("b"), lax.axis_index("c")
    gi = z * 2 + a
    gj = y * 4 + b * 2 + c
    a1, b1, c1 = 1 - a, 1 - b, 1 - c
    off_diag = gi != gj

    load_g = pltpu.make_async_copy(g_hbm, gt, in_sem.at[0])
    load_a = pltpu.make_async_copy(a_hbm, a_in, in_sem.at[1])
    load_g.start()
    load_a.start()

    def gx_of(s):
        i = lax.rem(gi + s, N)
        return i // 2, lax.rem(i, 2)

    def gy_of(j):
        return j // 4, lax.rem(j // 2, 2), lax.rem(j, 2)

    barrier = pltpu.get_barrier_semaphore()

    def greet(**where):
        pl.semaphore_signal(barrier, inc=1, device_id=where, device_id_type=MESH)

    zj, aj = gj // 2, lax.rem(gj, 2)

    @pl.when(off_diag)
    def _():
        for k in range(N):
            greet(z=zj, a=aj, y=k // 4, b=(k // 2) % 2, c=k % 2)

    for s in range(1, N):
        py, pb, pc = gy_of(lax.rem(gj + s, N))
        greet(y=py, b=pb, c=pc)
    for dz in (1, 2, 6, 7):
        greet(z=lax.rem(z + dz, 8))
    greet(a=a1)

    load_g.wait()
    GI[gj] = gt[...]
    pl.semaphore_wait(barrier, 35)

    sends = []

    def send(src, dst, rsem, **where):
        copy = pltpu.make_async_remote_copy(
            src_ref=src, dst_ref=dst, send_sem=send_sem.at[len(sends)], recv_sem=rsem,
            device_id=where, device_id_type=MESH,
        )
        copy.start()
        sends.append(copy)

    def arrived(ref, rsem):
        pltpu.make_async_remote_copy(
            src_ref=ref, dst_ref=ref, send_sem=gs_sem, recv_sem=rsem,
            device_id={"a": a1}, device_id_type=MESH,
        ).wait_recv()

    iy, ib, ic = gy_of(gi)
    for s in (8, 7, 9, 6, 10, 5, 11, 4, 12, 3, 13, 2, 14, 1, 15):
        pz, pa = gx_of(s)
        send(gt, GJ.at[gj], gj_sem.at[gj], z=pz, a=pa, y=iy, b=ib, c=ic)
    for s in (8, 7, 9, 6, 10, 5, 11, 4, 12, 3, 13, 2, 14, 1, 15):
        py, pb, pc = gy_of(lax.rem(gj + s, N))
        send(gt, GI.at[gj], gi_sem.at[gj], y=py, b=pb, c=pc)

    for s in range(1, N):
        k = lax.rem(gj + s, N)
        arrived(GI.at[k], gi_sem.at[k])

    @pl.when(off_diag)
    def _():
        for k in range(N):
            arrived(GJ.at[k], gj_sem.at[k])

    @pl.when(jnp.logical_not(off_diag))
    def _():
        GJ[...] = GI[...]

    load_a.wait()
    left = jnp.transpose(GI[...].reshape(N * KP, B))
    right = GJ[...].reshape(N * KP, B)
    lh, ll = split(left)
    rh, rl = split(right)
    full = jnp.dot(
        jnp.concatenate([lh, ll], axis=0), jnp.concatenate([rh, rl], axis=1),
        preferred_element_type=jnp.float32,
    )
    stat = 0.9 * a_in[...] + fold4(full) / float(N * KP)
    s_out[...] = stat
    R1[gj] = stat
    C1[gi] = stat

    def exchange(R, C, rsem, csem, rows):
        width = B // CH
        parts = [(h * width, width) for h in range(CH)]
        parts[-1] = (B - width, width + rows - B)
        chunks = range(CH)

        def row_ref(dy, bb, cc):
            k = lax.rem(y + dy, 4) * 4 + bb * 2 + cc
            return R.at[k], rsem.at[k]

        def col_ref(dz, aa, h):
            k = lax.rem(z + dz + 8, 8) * 2 + aa
            return C.at[k, pl.ds(*parts[h])], csem.at[k, h]

        def fwd(item, **where):
            ref, sem = item
            send(ref, ref, sem, **where)

        def got(item):
            arrived(*item)

        def zs(dz):
            return lax.rem(z + dz + 8, 8)

        def ys(dy):
            return lax.rem(y + dy, 4)

        def far(item, h, sign):
            fwd(item, z=zs(sign))
            if (h % 2 == 0) == (sign > 0):
                fwd(item, z=zs(2 * sign))

        late = [h for h in chunks if h < CH // 2]
        early = [h for h in chunks if h >= CH // 2]

        for h in chunks:
            fwd(col_ref(0, a, h), z=zs(2))
            fwd(col_ref(0, a, h), z=zs(-2))
            fwd(col_ref(0, a, h), a=a1)
        for h in chunks:
            fwd(col_ref(0, a, h), z=zs(1))
            fwd(col_ref(0, a, h), z=zs(-1))
        mine = row_ref(0, b, c)
        fwd(mine, b=b1)
        for dy in (1, 3, 2):
            fwd(mine, y=ys(dy))
        fwd(mine, c=c1)

        for h in chunks:
            got(col_ref(0, a1, h))
            if h in late:
                fwd(col_ref(0, a1, h), z=zs(1))
                fwd(col_ref(0, a1, h), z=zs(-1))
        for h in chunks:
            for sign in (1, -1):
                item = col_ref(-2 * sign, a, h)
                got(item)
                fwd(item, a=a1)
                far(item, h, sign)
        for dy in (1, 3):
            got(row_ref(dy, b, c))
            fwd(row_ref(dy, b, c), c=c1)
        other = row_ref(0, b1, c)
        got(other)
        for dy in (1, 3, 2):
            fwd(other, y=ys(dy))
        fwd(other, c=c1)
        for h in chunks:
            for dz in (-1, 1):
                got(col_ref(dz, a, h))
                if h in early:
                    fwd(col_ref(dz, a, h), a=a1)
        got(row_ref(2, b, c))
        fwd(row_ref(2, b, c), c=c1)
        for h in chunks:
            for sign in (1, -1):
                item = col_ref(-2 * sign, a1, h)
                got(item)
                if h in early:
                    far(item, h, sign)
        for h in chunks:
            for dz in (-3, 3, 4):
                got(col_ref(dz, a, h))
                if h in late:
                    fwd(col_ref(dz, a, h), a=a1)
        for dy in (1, 3, 2):
            got(row_ref(dy, b1, c))
            fwd(row_ref(dy, b1, c), c=c1)
        for dy, bb in ((0, b), (1, b), (3, b), (0, b1), (2, b), (1, b1), (3, b1), (2, b1)):
            got(row_ref(dy, bb, c1))
        for dz in (-1, 1, -3, 3, 4):
            for h in chunks:
                got(col_ref(dz, a1, h))

    exchange(R1, C1, r1_sem, c1_sem, B)

    def strips(R, k):
        rows = jnp.concatenate([R[2 * k], R[2 * k + 1]], axis=1)
        hi, lo = split(rows)
        return jnp.concatenate([hi, lo], axis=0)

    def columns(C, k):
        rows = jnp.concatenate([C[2 * k, :B], C[2 * k + 1, :B]], axis=0)
        hi, lo = split(rows)
        return jnp.concatenate([hi, lo], axis=1)

    squares = jnp.zeros((PAD, B), jnp.float32)
    total = jnp.zeros((2 * B, 2 * B), jnp.float32)
    for k in range(8):
        total = total + jnp.dot(strips(R1, k), columns(C1, k), preferred_element_type=jnp.float32)
    for k in range(N):
        block = R1[k]
        squares = squares + jnp.sum((block * block).reshape(B // PAD, PAD, B), axis=0)
    mid = fold4(total)
    R2[gj] = mid
    C2[gi, :B] = mid
    C2[gi, B:] = squares

    exchange(R2, C2, r2_sem, c2_sem, B + PAD)

    wide = jnp.zeros((2 * B, 4 * B), jnp.float32)
    for k in range(8):
        both = jnp.concatenate([columns(C1, k), columns(C2, k)], axis=1)
        wide = wide + jnp.dot(strips(R2, k), both, preferred_element_type=jnp.float32)
    cube = fold4(wide[:, : 2 * B])
    quad = fold4(wide[:, 2 * B:])
    squares = jnp.zeros((PAD, B), jnp.float32)
    for k in range(N):
        squares = squares + C2[k, B:]
    whole = jnp.sum(squares, keepdims=True)
    inv = 1.0 / (2.0 * jnp.sqrt(whole / float(N * B)))
    rows = lax.broadcasted_iota(jnp.int32, (B, B), 0) + gi * B
    cols = lax.broadcasted_iota(jnp.int32, (B, B), 1) + gj * B
    eye = jnp.where(rows == cols, A0, 0.0)
    tail = A2 * R2[gj] + inv * (A3 * cube + inv * (A4 * quad))
    r_out[...] = eye + inv * (A1 * R1[gj] + inv * tail)

    for copy in sends:
        copy.wait_send()


def local(gradient, stat_old):
    f32 = jnp.float32
    dma = pltpu.SemaphoreType.DMA
    return pl.pallas_call(
        kernel,
        out_shape=(jax.ShapeDtypeStruct((B, B), f32), jax.ShapeDtypeStruct((B, B), f32)),
        in_specs=[pl.BlockSpec(memory_space=pl.ANY)] * 2,
        out_specs=[pl.BlockSpec(memory_space=pltpu.VMEM)] * 2,
        scratch_shapes=[
            pltpu.VMEM((B, B), f32),
            pltpu.VMEM((KP, B), f32),
            pltpu.VMEM((N, KP, B), f32),
            pltpu.VMEM((N, KP, B), f32),
            pltpu.VMEM((N, B, B), f32),
            pltpu.VMEM((N, B, B), f32),
            pltpu.VMEM((N, B, B), f32),
            pltpu.VMEM((N, B + PAD, B), f32),
            dma((2,)),
            dma((N,)),
            dma((N,)),
            dma,
            dma((N,)),
            dma((N, CH)),
            dma((N,)),
            dma((N, CH)),
            dma((256,)),
        ],
        compiler_params=pltpu.CompilerParams(collective_id=0, has_side_effects=True),
    )(gradient.T, stat_old)


def solution(mesh):
    torus = Mesh(mesh.devices.reshape(8, 2, 4, 2, 2), ("z", "a", "y", "b", "c"))
    return jax.shard_map(
        local, mesh=torus, in_specs=(P(GX, GY), P(GX, GY)),
        out_specs=(P(GX, GY), P(GX, GY)), check_vma=False,
    )
```

```python
import functools

import jax
import jax.numpy as jnp
from jax import lax
from jax.experimental import pallas as pl
from jax.experimental.pallas import tpu as pltpu
from jax.sharding import Mesh
from jax.sharding import PartitionSpec as P

MESH = pl.DeviceIdType.MESH
GX = ("z", "a")
GY = ("y", "b", "c")
B = 128
CH = 4
PAD = 8
KP = 32
N = 16

A0, A1, A2, A3, A4 = 2.25, -2.4375, 1.6875, -0.5625, 0.0625


def split(x):
    hi = x.astype(jnp.bfloat16)
    lo = (x - hi.astype(jnp.float32)).astype(jnp.bfloat16)
    return hi, lo


def fold4(full):
    return (full[:B, :B] + full[B:, :B]) + (full[:B, B:] + full[B:, B:])


def kernel(
    g_hbm, a_hbm, s_out, r_out,
    a_in, gt, GI, GJ, R1, C1, R2, C2,
    in_sem, gi_sem, gj_sem, gs_sem, r1_sem, c1_sem, r2_sem, c2_sem, send_sem,
):
    z, a = lax.axis_index("z"), lax.axis_index("a")
    y, b, c = lax.axis_index("y"), lax.axis_index("b"), lax.axis_index("c")
    gi = z * 2 + a
    gj = y * 4 + b * 2 + c
    a1, b1, c1 = 1 - a, 1 - b, 1 - c
    off_diag = gi != gj

    load_g = pltpu.make_async_copy(g_hbm, gt, in_sem.at[0])
    load_a = pltpu.make_async_copy(a_hbm, a_in, in_sem.at[1])
    load_g.start()
    load_a.start()

    def gx_of(s):
        i = lax.rem(gi + s, N)
        return i // 2, lax.rem(i, 2)

    def gy_of(j):
        return j // 4, lax.rem(j // 2, 2), lax.rem(j, 2)

    barrier = pltpu.get_barrier_semaphore()

    def greet(**where):
        pl.semaphore_signal(barrier, inc=1, device_id=where, device_id_type=MESH)

    zj, aj = gj // 2, lax.rem(gj, 2)

    @pl.when(off_diag)
    def _():
        for k in range(N):
            greet(z=zj, a=aj, y=k // 4, b=(k // 2) % 2, c=k % 2)

    for s in range(1, N):
        py, pb, pc = gy_of(lax.rem(gj + s, N))
        greet(y=py, b=pb, c=pc)
    for dz in (1, 2, 6, 7):
        greet(z=lax.rem(z + dz, 8))
    greet(a=a1)

    load_g.wait()
    GI[gj] = gt[...]
    pl.semaphore_wait(barrier, 35)

    sends = []

    def send(src, dst, rsem, **where):
        copy = pltpu.make_async_remote_copy(
            src_ref=src, dst_ref=dst, send_sem=send_sem.at[len(sends)], recv_sem=rsem,
            device_id=where, device_id_type=MESH,
        )
        copy.start()
        sends.append(copy)

    def arrived(ref, rsem):
        pltpu.make_async_remote_copy(
            src_ref=ref, dst_ref=ref, send_sem=gs_sem, recv_sem=rsem,
            device_id={"a": a1}, device_id_type=MESH,
        ).wait_recv()

    iy, ib, ic = gy_of(gi)
    for s in (8, 7, 9, 6, 10, 5, 11, 4, 12, 3, 13, 2, 14, 1, 15):
        pz, pa = gx_of(s)
        send(gt, GJ.at[gj], gj_sem.at[gj], z=pz, a=pa, y=iy, b=ib, c=ic)
    for s in (8, 7, 9, 6, 10, 5, 11, 4, 12, 3, 13, 2, 14, 1, 15):
        py, pb, pc = gy_of(lax.rem(gj + s, N))
        send(gt, GI.at[gj], gi_sem.at[gj], y=py, b=pb, c=pc)

    for s in range(1, N):
        k = lax.rem(gj + s, N)
        arrived(GI.at[k], gi_sem.at[k])

    @pl.when(off_diag)
    def _():
        for k in range(N):
            arrived(GJ.at[k], gj_sem.at[k])

    @pl.when(jnp.logical_not(off_diag))
    def _():
        GJ[...] = GI[...]

    load_a.wait()
    left = jnp.transpose(GI[...].reshape(N * KP, B))
    right = GJ[...].reshape(N * KP, B)
    lh, ll = split(left)
    rh, rl = split(right)
    full = jnp.dot(
        jnp.concatenate([lh, ll], axis=0), jnp.concatenate([rh, rl], axis=1),
        preferred_element_type=jnp.float32,
    )
    stat = 0.9 * a_in[...] + fold4(full) / float(N * KP)
    s_out[...] = stat
    R1[gj] = stat
    C1[gi] = stat

    def exchange(R, C, rsem, csem, rows):
        width = B // CH
        parts = [(h * width, width) for h in range(CH)]
        parts[-1] = (B - width, width + rows - B)
        chunks = range(CH)

        def row_ref(dy, bb, cc):
            k = lax.rem(y + dy, 4) * 4 + bb * 2 + cc
            return R.at[k], rsem.at[k]

        def col_ref(dz, aa, h):
            k = lax.rem(z + dz + 8, 8) * 2 + aa
            return C.at[k, pl.ds(*parts[h])], csem.at[k, h]

        def fwd(item, **where):
            ref, sem = item
            send(ref, ref, sem, **where)

        def got(item):
            arrived(*item)

        def zs(dz):
            return lax.rem(z + dz + 8, 8)

        def ys(dy):
            return lax.rem(y + dy, 4)

        def far(item, h, sign):
            fwd(item, z=zs(sign))
            if (h % 2 == 0) == (sign > 0):
                fwd(item, z=zs(2 * sign))

        late = [h for h in chunks if h < CH // 2]
        early = [h for h in chunks if h >= CH // 2]

        for h in chunks:
            fwd(col_ref(0, a, h), z=zs(2))
            fwd(col_ref(0, a, h), z=zs(-2))
            fwd(col_ref(0, a, h), a=a1)
        for h in chunks:
            fwd(col_ref(0, a, h), z=zs(1))
            fwd(col_ref(0, a, h), z=zs(-1))
        mine = row_ref(0, b, c)
        fwd(mine, b=b1)
        for dy in (1, 3, 2):
            fwd(mine, y=ys(dy))
        fwd(mine, c=c1)

        for h in chunks:
            got(col_ref(0, a1, h))
            if h in late:
                fwd(col_ref(0, a1, h), z=zs(1))
                fwd(col_ref(0, a1, h), z=zs(-1))
        for h in chunks:
            for sign in (1, -1):
                item = col_ref(-2 * sign, a, h)
                got(item)
                fwd(item, a=a1)
                far(item, h, sign)
        for dy in (1, 3):
            got(row_ref(dy, b, c))
            fwd(row_ref(dy, b, c), c=c1)
        other = row_ref(0, b1, c)
        got(other)
        for dy in (1, 3, 2):
            fwd(other, y=ys(dy))
        fwd(other, c=c1)
        for h in chunks:
            for dz in (-1, 1):
                got(col_ref(dz, a, h))
                if h in early:
                    fwd(col_ref(dz, a, h), a=a1)
        got(row_ref(2, b, c))
        fwd(row_ref(2, b, c), c=c1)
        for h in chunks:
            for sign in (1, -1):
                item = col_ref(-2 * sign, a1, h)
                got(item)
                if h in early:
                    far(item, h, sign)
        for h in chunks:
            for dz in (-3, 3, 4):
                got(col_ref(dz, a, h))
                if h in late:
                    fwd(col_ref(dz, a, h), a=a1)
        for dy in (1, 3, 2):
            got(row_ref(dy, b1, c))
            fwd(row_ref(dy, b1, c), c=c1)
        for dy, bb in ((0, b), (1, b), (3, b), (0, b1), (2, b), (1, b1), (3, b1), (2, b1)):
            got(row_ref(dy, bb, c1))
        for dz in (-1, 1, -3, 3, 4):
            for h in chunks:
                got(col_ref(dz, a1, h))

    exchange(R1, C1, r1_sem, c1_sem, B)

    def strips(R, k):
        rows = jnp.concatenate([R[2 * k], R[2 * k + 1]], axis=1)
        hi, lo = split(rows)
        return jnp.concatenate([hi, lo], axis=0)

    def columns(C, k):
        rows = jnp.concatenate([C[2 * k, :B], C[2 * k + 1, :B]], axis=0)
        hi, lo = split(rows)
        return jnp.concatenate([hi, lo], axis=1)

    squares = jnp.zeros((PAD, B), jnp.float32)
    total = jnp.zeros((2 * B, 2 * B), jnp.float32)
    for k in range(8):
        total = total + jnp.dot(strips(R1, k), columns(C1, k), preferred_element_type=jnp.float32)
    for k in range(N):
        block = R1[k]
        squares = squares + jnp.sum((block * block).reshape(B // PAD, PAD, B), axis=0)
    mid = fold4(total)
    R2[gj] = mid
    C2[gi, :B] = mid
    C2[gi, B:] = squares

    exchange(R2, C2, r2_sem, c2_sem, B + PAD)

    wide = jnp.zeros((2 * B, 4 * B), jnp.float32)
    for k in range(8):
        both = jnp.concatenate([columns(C1, k), columns(C2, k)], axis=1)
        wide = wide + jnp.dot(strips(R2, k), both, preferred_element_type=jnp.float32)
    cube = fold4(wide[:, : 2 * B])
    quad = fold4(wide[:, 2 * B:])
    squares = jnp.zeros((PAD, B), jnp.float32)
    for k in range(N):
        squares = squares + C2[k, B:]
    whole = jnp.sum(squares, keepdims=True)
    inv = 1.0 / (2.0 * jnp.sqrt(whole / float(N * B)))
    rows = lax.broadcasted_iota(jnp.int32, (B, B), 0) + gi * B
    cols = lax.broadcasted_iota(jnp.int32, (B, B), 1) + gj * B
    eye = jnp.where(rows == cols, A0, 0.0)
    tail = A2 * R2[gj] + inv * (A3 * cube + inv * (A4 * quad))
    r_out[...] = eye + inv * (A1 * R1[gj] + inv * tail)

    for copy in sends:
        copy.wait_send()


def local(gradient, stat_old):
    f32 = jnp.float32
    dma = pltpu.SemaphoreType.DMA
    return pl.pallas_call(
        kernel,
        out_shape=(pltpu.VMEM((B, B), f32), pltpu.VMEM((B, B), f32)),
        in_specs=[pl.BlockSpec(memory_space=pl.ANY)] * 2,
        out_specs=[pl.BlockSpec(memory_space=pltpu.VMEM)] * 2,
        scratch_shapes=[
            pltpu.VMEM((B, B), f32),
            pltpu.VMEM((KP, B), f32),
            pltpu.VMEM((N, KP, B), f32),
            pltpu.VMEM((N, KP, B), f32),
            pltpu.VMEM((N, B, B), f32),
            pltpu.VMEM((N, B, B), f32),
            pltpu.VMEM((N, B, B), f32),
            pltpu.VMEM((N, B + PAD, B), f32),
            dma((2,)),
            dma((N,)),
            dma((N,)),
            dma,
            dma((N,)),
            dma((N, CH)),
            dma((N,)),
            dma((N, CH)),
            dma((256,)),
        ],
        compiler_params=pltpu.CompilerParams(collective_id=0, has_side_effects=True),
    )(gradient.T, stat_old)


def solution(mesh):
    torus = Mesh(mesh.devices.reshape(8, 2, 4, 2, 2), ("z", "a", "y", "b", "c"))
    return jax.shard_map(
        local, mesh=torus, in_specs=(P(GX, GY), P(GX, GY)),
        out_specs=(P(GX, GY), P(GX, GY)), check_vma=False,
    )
```

```python
import jax
import jax.numpy as jnp
from jax import lax
from jax.experimental import pallas as pl
from jax.experimental.pallas import tpu as pltpu
from jax.sharding import Mesh
from jax.sharding import PartitionSpec as P

MESH = pl.DeviceIdType.MESH
GX = ("z", "a")
GY = ("y", "b", "c")
B = 128
CH = 2
RH = 2
PAD = 8
KP = 32
N = 16

A0, A1, A2, A3, A4 = 2.25, -2.4375, 1.6875, -0.5625, 0.0625


def split(x):
    hi = x.astype(jnp.bfloat16)
    lo = (x - hi.astype(jnp.float32)).astype(jnp.bfloat16)
    return hi, lo


def fold4(full):
    return (full[:B, :B] + full[B:, :B]) + (full[:B, B:] + full[B:, B:])


def kernel(
    g_hbm, a_hbm, s_out, r_out,
    a_in, gt, GI, GJ, R1, C1, R2, C2, a_new, s_new, r_own, r_new,
    in_sem, gi_sem, gj_sem, gs_sem, down_sem, swap_sem, r1_sem, c1_sem, r2_sem, c2_sem, send_sem,
):
    z, a = lax.axis_index("z"), lax.axis_index("a")
    y, b, c = lax.axis_index("y"), lax.axis_index("b"), lax.axis_index("c")
    a1, b1, c1 = 1 - a, 1 - b, 1 - c
    x = 2 * b + a
    gi = z * 2 + c
    gj = y * 4 + x
    own = c * 8 + y * 2 + b
    home = z == 2 * y + b
    swaps = a != c

    load_g = pltpu.make_async_copy(g_hbm, gt, in_sem.at[0])
    load_a = pltpu.make_async_copy(a_hbm, a_in, in_sem.at[1])
    load_g.start()
    load_a.start()

    barrier = pltpu.get_barrier_semaphore()

    def greet(**where):
        pl.semaphore_signal(barrier, inc=1, device_id=where, device_id_type=MESH)

    def zs(dz):
        return lax.rem(z + dz + 8, 8)

    def ys(dy):
        return lax.rem(y + dy + 4, 4)

    def xs(dx):
        to = lax.rem(x + dx + 4, 4)
        return {"b": to // 2, "a": lax.rem(to, 2)}

    def place(slot):
        return {"y": (slot % 8) // 2, "b": slot % 2, "c": slot // 8}

    @pl.when(c == 0)
    def _():
        for slot in range(N):
            @pl.when(jnp.logical_not(jnp.logical_and(home, own == slot)))
            def _():
                greet(z=2 * y + b, **place(slot))

    for slot in range(N):
        @pl.when(jnp.logical_not(jnp.logical_and(a == c, own == slot)))
        def _():
            greet(a=c, **place(slot))

    @pl.when(swaps)
    def _():
        greet(a=a1, c=c1)

    @pl.when(c == 1)
    def _():
        greet(c=0)

    for dz in (2, -2, 1, -1):
        greet(z=zs(dz))
    for d in (2, 1, -1):
        greet(y=ys(d))
        greet(**xs(d))
    greet(c=c1)
    alike = jnp.where(a == c, 1, 0)
    at_home = jnp.where(home, 1, 0)
    expected = 36 - 2 * alike + (1 - c) - (1 - c) * at_home

    load_g.wait()
    pl.semaphore_wait(barrier, expected)

    sends = []

    def send(src, dst, rsem, cond=None, **where):
        copy = pltpu.make_async_remote_copy(
            src_ref=src, dst_ref=dst, send_sem=send_sem.at[len(sends)], recv_sem=rsem,
            device_id=where, device_id_type=MESH,
        )
        if cond is None:
            copy.start()
        else:
            pl.when(cond)(copy.start)
        sends.append((copy, cond))

    def arrived(ref, rsem):
        pltpu.make_async_remote_copy(
            src_ref=ref, dst_ref=ref, send_sem=gs_sem, recv_sem=rsem,
            device_id={"c": c1}, device_id_type=MESH,
        ).wait_recv()

    col_y, col_b = z // 2, lax.rem(z, 2)
    for dz in (4, 3, 5, 2, 6, 1, 7):
        send(gt, GJ.at[own], gj_sem.at[own], z=zs(dz), y=col_y, b=col_b, c=0)
    away = jnp.logical_not(jnp.logical_and(home, c == 0))
    send(gt, GJ.at[own], gj_sem.at[own], away, y=col_y, b=col_b, c=0)
    for dx in (2, 1, -1, 0):
        for dy in (2, 1, -1, 0):
            cond = swaps if dx == 0 and dy == 0 else None
            to = xs(dx)
            send(gt, GI.at[own], gi_sem.at[own], cond, y=ys(dy), b=to["b"], a=to["a"], c=a)

    load_a.wait()
    send(a_in, a_new, swap_sem.at[0], swaps, a=a1, c=c1)

    @pl.when(a == c)
    def _():
        GI[own] = gt[...]
        a_new[...] = a_in[...]

    @pl.when(jnp.logical_and(home, c == 0))
    def _():
        GJ[own] = gt[...]

    lower = GJ.at[pl.ds(0, 8)]
    upper = GJ.at[pl.ds(8, 8)]
    for group, part in enumerate((lower, upper)):
        @pl.when(c == 0)
        def _():
            for slot in range(8 * group, 8 * group + 8):
                @pl.when(jnp.logical_not(jnp.logical_and(home, own == slot)))
                def _():
                    arrived(GJ.at[slot], gj_sem.at[slot])

        send(part, part, down_sem.at[group], c == 0, c=c1)

    for t in range(1, N):
        slot = lax.rem(own + t, N)
        arrived(GI.at[slot], gi_sem.at[slot])

    @pl.when(swaps)
    def _():
        arrived(GI.at[own], gi_sem.at[own])
        arrived(a_new, swap_sem.at[0])

    @pl.when(c == 1)
    def _():
        arrived(lower, down_sem.at[0])
        arrived(upper, down_sem.at[1])

    left = jnp.transpose(GI[...].reshape(N * KP, B))
    right = GJ[...].reshape(N * KP, B)
    lh, ll = split(left)
    rh, rl = split(right)
    full = jnp.dot(
        jnp.concatenate([lh, ll], axis=0), jnp.concatenate([rh, rl], axis=1),
        preferred_element_type=jnp.float32,
    )
    stat = 0.9 * a_new[...] + fold4(full) / float(N * KP)
    R1[gj] = stat
    C1[gi] = stat

    def exchange(R, C, rsem, csem, rows, extra):
        width = B // CH
        parts = [(h * width, width) for h in range(CH)]
        parts[-1] = (B - width, width + rows - B)
        chunks = range(CH)
        tall = B // RH
        pairs = [(h, h + RH // 2) for h in range(RH // 2)]

        def row_ref(dy, dx, h):
            k = ys(dy) * 4 + lax.rem(x + dx + 4, 4)
            return R.at[k, pl.ds(h * tall, tall)], rsem.at[k, h]

        def col_ref(dz, core, h):
            k = zs(dz) * 2 + core
            return C.at[k, pl.ds(*parts[h])], csem.at[k, h]

        def fwd(item, **where):
            ref, sem = item
            send(ref, ref, sem, **where)

        def got(item):
            arrived(*item)

        for dz in (2, -2, 1, -1):
            for h in chunks:
                fwd(col_ref(0, c, h), z=zs(dz))
        for h, v in pairs:
            for d in (2, 1, -1):
                fwd(row_ref(0, 0, h), **xs(d))
                fwd(row_ref(0, 0, v), y=ys(d))
        for h in chunks:
            fwd(col_ref(0, c, h), c=c1)
        for h, v in pairs:
            for d in (2, 1, -1):
                fwd(row_ref(0, 0, v), **xs(d))
                fwd(row_ref(0, 0, h), y=ys(d))
        extra()

        for h, v in pairs:
            for d in (1, -1, 2):
                got(row_ref(0, d, h))
                for e in (2, 1, -1):
                    fwd(row_ref(0, d, h), y=ys(e))
                got(row_ref(d, 0, v))
                for e in (2, 1, -1):
                    fwd(row_ref(d, 0, v), **xs(e))
        for h in chunks:
            for sign in (1, -1):
                item = col_ref(-2 * sign, c, h)
                got(item)
                fwd(item, z=zs(sign))
                if (h % 2 == 0) == (sign > 0):
                    fwd(item, z=zs(2 * sign))
                fwd(item, c=c1)
        for h in chunks:
            for dz in (-1, 1):
                got(col_ref(dz, c, h))
                fwd(col_ref(dz, c, h), c=c1)
        for h in chunks:
            for dz in (-3, 3, 4):
                got(col_ref(dz, c, h))
                fwd(col_ref(dz, c, h), c=c1)
        for h, v in pairs:
            for d in (1, -1, 2):
                got(row_ref(0, d, v))
                got(row_ref(d, 0, h))
                for e in (1, -1, 2):
                    got(row_ref(e, d, h))
                    got(row_ref(d, e, v))
        for h in chunks:
            for dz in (0, -1, 1, -2, 2, -3, 3, 4):
                got(col_ref(dz, c1, h))

    def give_stat():
        send(R1.at[gj], s_new, swap_sem.at[1], swaps, a=a1, c=c1)

    exchange(R1, C1, r1_sem, c1_sem, B, give_stat)

    def strips(R, k):
        rows = jnp.concatenate([R[2 * k], R[2 * k + 1]], axis=1)
        hi, lo = split(rows)
        return jnp.concatenate([hi, lo], axis=0)

    def columns(C, k):
        rows = jnp.concatenate([C[2 * k, :B], C[2 * k + 1, :B]], axis=0)
        hi, lo = split(rows)
        return jnp.concatenate([hi, lo], axis=1)

    squares = jnp.zeros((PAD, B), jnp.float32)
    total = jnp.zeros((2 * B, 2 * B), jnp.float32)
    for k in range(8):
        total = total + jnp.dot(strips(R1, k), columns(C1, k), preferred_element_type=jnp.float32)
    for k in range(N):
        block = R1[k]
        squares = squares + jnp.sum((block * block).reshape(B // PAD, PAD, B), axis=0)
    mid = fold4(total)
    R2[gj] = mid
    C2[gi, :B] = mid
    C2[gi, B:] = squares

    def keep_stat():
        @pl.when(swaps)
        def _():
            arrived(s_new, swap_sem.at[1])
            s_out[...] = s_new[...]

        @pl.when(a == c)
        def _():
            s_out[...] = R1[gj]

    exchange(R2, C2, r2_sem, c2_sem, B + PAD, keep_stat)

    wide = jnp.zeros((2 * B, 4 * B), jnp.float32)
    for k in range(8):
        both = jnp.concatenate([columns(C1, k), columns(C2, k)], axis=1)
        wide = wide + jnp.dot(strips(R2, k), both, preferred_element_type=jnp.float32)
    cube = fold4(wide[:, : 2 * B])
    quad = fold4(wide[:, 2 * B:])
    squares = jnp.zeros((PAD, B), jnp.float32)
    for k in range(N):
        squares = squares + C2[k, B:]
    whole = jnp.sum(squares, keepdims=True)
    inv = 1.0 / (2.0 * jnp.sqrt(whole / float(N * B)))
    rows = lax.broadcasted_iota(jnp.int32, (B, B), 0) + gi * B
    cols = lax.broadcasted_iota(jnp.int32, (B, B), 1) + gj * B
    eye = jnp.where(rows == cols, A0, 0.0)
    tail = A2 * R2[gj] + inv * (A3 * cube + inv * (A4 * quad))
    r_own[...] = eye + inv * (A1 * R1[gj] + inv * tail)
    send(r_own, r_new, swap_sem.at[2], swaps, a=a1, c=c1)

    @pl.when(swaps)
    def _():
        arrived(r_new, swap_sem.at[2])
        r_out[...] = r_new[...]

    @pl.when(a == c)
    def _():
        r_out[...] = r_own[...]

    for copy, cond in sends:
        if cond is None:
            copy.wait_send()
        else:
            pl.when(cond)(copy.wait_send)


def local(gradient, stat_old):
    f32 = jnp.float32
    dma = pltpu.SemaphoreType.DMA
    tile = pltpu.VMEM((B, B), f32)
    pieces = pltpu.VMEM((N, KP, B), f32)
    strip = pltpu.VMEM((N, B, B), f32)
    return pl.pallas_call(
        kernel,
        out_shape=(pltpu.VMEM((B, B), f32), pltpu.VMEM((B, B), f32)),
        in_specs=[pl.BlockSpec(memory_space=pl.ANY)] * 2,
        out_specs=[pl.BlockSpec(memory_space=pltpu.VMEM)] * 2,
        scratch_shapes=[
            tile, pltpu.VMEM((KP, B), f32), pieces, pieces,
            strip, strip, strip, pltpu.VMEM((N, B + PAD, B), f32),
            tile, tile, tile, tile,
            dma((2,)), dma((N,)), dma((N,)), dma, dma((2,)), dma((3,)),
            dma((N, RH)), dma((N, CH)), dma((N, RH)), dma((N, CH)), dma((256,)),
        ],
        compiler_params=pltpu.CompilerParams(collective_id=0, has_side_effects=True),
    )(gradient.T, stat_old)


def solution(mesh):
    torus = Mesh(mesh.devices.reshape(8, 2, 4, 2, 2), ("z", "a", "y", "b", "c"))
    return jax.shard_map(
        local, mesh=torus, in_specs=(P(GX, GY), P(GX, GY)),
        out_specs=(P(GX, GY), P(GX, GY)), check_vma=False,
    )
```

```python
import jax
import jax.numpy as jnp
from jax import lax
from jax.experimental import pallas as pl
from jax.experimental.pallas import tpu as pltpu
from jax.sharding import Mesh
from jax.sharding import PartitionSpec as P

MESH = pl.DeviceIdType.MESH
GX = ("z", "a")
GY = ("y", "b", "c")
B = 128
CH = 2
RH = 4
EARLY = (0, -1, 1, -2, 2)
LATE = (-3, 3, 4)
PAD = 8
KP = 32
N = 16

A0, A1, A2, A3, A4 = 2.25, -2.4375, 1.6875, -0.5625, 0.0625


def split(x):
    hi = x.astype(jnp.bfloat16)
    lo = (x - hi.astype(jnp.float32)).astype(jnp.bfloat16)
    return hi, lo


def fold4(full):
    return (full[:B, :B] + full[B:, :B]) + (full[:B, B:] + full[B:, B:])


def kernel(
    g_hbm, a_hbm, s_out, r_out,
    a_in, gt, GI, GJ, R1, C1, R2, C2, CB, a_new, s_new, r_own, r_new,
    in_sem, gi_sem, gj_sem, gs_sem, down_sem, swap_sem, piece_sem, send_sem, *gather_sems,
):
    z, a = lax.axis_index("z"), lax.axis_index("a")
    y, b, c = lax.axis_index("y"), lax.axis_index("b"), lax.axis_index("c")
    a1, b1, c1 = 1 - a, 1 - b, 1 - c
    x = 2 * b + a
    gi = z * 2 + c
    gj = y * 4 + x
    own = c * 8 + y * 2 + b
    home = z == 2 * y + b
    swaps = a != c

    sems1, sems2 = gather_sems[:7], gather_sems[7:]
    load_g = pltpu.make_async_copy(g_hbm, gt, in_sem.at[0])
    load_a = pltpu.make_async_copy(a_hbm, a_in, in_sem.at[1])
    load_g.start()
    load_a.start()

    barrier = pltpu.get_barrier_semaphore()

    def greet(**where):
        pl.semaphore_signal(barrier, inc=1, device_id=where, device_id_type=MESH)

    def zs(dz):
        return lax.rem(z + dz + 8, 8)

    def ys(dy):
        return lax.rem(y + dy + 4, 4)

    def xs(dx):
        to = lax.rem(x + dx + 4, 4)
        return {"b": to // 2, "a": lax.rem(to, 2)}

    def place(slot):
        return {"y": (slot % 8) // 2, "b": slot % 2, "c": slot // 8}

    @pl.when(c == 0)
    def _():
        for slot in range(N):
            @pl.when(jnp.logical_not(jnp.logical_and(home, own == slot)))
            def _():
                greet(z=2 * y + b, **place(slot))

    for slot in range(N):
        @pl.when(jnp.logical_not(jnp.logical_and(a == c, own == slot)))
        def _():
            greet(a=c, **place(slot))

    @pl.when(swaps)
    def _():
        greet(a=a1, c=c1)

    @pl.when(c == 1)
    def _():
        greet(c=0)

    for dz in (2, -2, 1, -1):
        greet(z=zs(dz))
    for d in (2, 1, -1):
        greet(y=ys(d))
        greet(**xs(d))
    greet(c=c1)
    alike = jnp.where(a == c, 1, 0)
    at_home = jnp.where(home, 1, 0)
    expected = 36 - 2 * alike + (1 - c) - (1 - c) * at_home

    load_g.wait()
    pl.semaphore_wait(barrier, expected)

    sends = []

    def start(src, dst, ssem, rsem, **where):
        copy = pltpu.make_async_remote_copy(
            src_ref=src, dst_ref=dst, send_sem=ssem, recv_sem=rsem,
            device_id=where, device_id_type=MESH,
        )
        copy.start()

    def send(src, dst, rsem, cond, **where):
        copy = pltpu.make_async_remote_copy(
            src_ref=src, dst_ref=dst, send_sem=send_sem.at[len(sends)], recv_sem=rsem,
            device_id=where, device_id_type=MESH,
        )
        pl.when(cond)(copy.start)
        sends.append((copy, cond))

    def left_here(ref, ssem):
        pltpu.make_async_remote_copy(
            src_ref=ref, dst_ref=ref, send_sem=ssem, recv_sem=gs_sem,
            device_id={"c": c1}, device_id_type=MESH,
        ).wait_send()

    def arrived(ref, rsem):
        pltpu.make_async_remote_copy(
            src_ref=ref, dst_ref=ref, send_sem=gs_sem, recv_sem=rsem,
            device_id={"c": c1}, device_id_type=MESH,
        ).wait_recv()

    col_y, col_b = z // 2, lax.rem(z, 2)
    for dz in (4, 3, 5, 2, 6, 1, 7):
        start(gt, GJ.at[own], piece_sem, gj_sem.at[c], z=zs(dz), y=col_y, b=col_b, c=0)
    away = jnp.logical_not(jnp.logical_and(home, c == 0))
    send(gt, GJ.at[own], gj_sem.at[c], away, y=col_y, b=col_b, c=0)
    for dx in (2, 1, -1, 0):
        for dy in (2, 1, -1, 0):
            if dx or dy:
                to = xs(dx)
                start(gt, GI.at[own], piece_sem, gi_sem, y=ys(dy), b=to["b"], a=to["a"], c=a)
    send(gt, GI.at[own], gi_sem, swaps, c=a)

    load_a.wait()
    send(a_in, a_new, swap_sem.at[0], swaps, a=a1, c=c1)

    @pl.when(a == c)
    def _():
        GI[own] = gt[...]
        a_new[...] = a_in[...]

    @pl.when(jnp.logical_and(home, c == 0))
    def _():
        GJ[own] = gt[...]

    lower = GJ.at[pl.ds(0, 8)]
    upper = GJ.at[pl.ds(8, 8)]

    @pl.when(c == 0)
    def _():
        @pl.when(home)
        def _():
            arrived(GJ.at[pl.ds(0, 7)], gj_sem.at[0])

        @pl.when(jnp.logical_not(home))
        def _():
            arrived(lower, gj_sem.at[0])

    send(lower, lower, down_sem.at[0], c == 0, c=c1)

    @pl.when(c == 0)
    def _():
        arrived(upper, gj_sem.at[1])

    send(upper, upper, down_sem.at[1], c == 0, c=c1)

    @pl.when(a == c)
    def _():
        arrived(GI.at[pl.ds(0, N - 1)], gi_sem)

    @pl.when(swaps)
    def _():
        arrived(GI, gi_sem)
        arrived(a_new, swap_sem.at[0])

    @pl.when(c == 1)
    def _():
        arrived(lower, down_sem.at[0])
        arrived(upper, down_sem.at[1])

    left = jnp.transpose(GI[...].reshape(N * KP, B))
    right = GJ[...].reshape(N * KP, B)
    lh, ll = split(left)
    rh, rl = split(right)
    full = jnp.dot(
        jnp.concatenate([lh, ll], axis=0), jnp.concatenate([rh, rl], axis=1),
        preferred_element_type=jnp.float32,
    )
    stat = 0.9 * a_new[...] + fold4(full) / float(N * KP)
    R1[gj] = stat
    C1[gi] = stat

    def exchange(R, C, sems, rows, extra, ready):
        width = B // CH
        parts = [(h * width, width) for h in range(CH)]
        parts[-1] = (B - width, width + rows - B)
        chunks = range(CH)
        tall = B // RH
        pairs = [(h, h + RH // 2) for h in range(RH // 2)]
        leg_sem, rest_sem, far_sem, block_sem, twin_sem, row_sent, col_sent = sems

        def row_ref(dy, dx, h):
            k = ys(dy) * 4 + lax.rem(x + dx + 4, 4)
            return R.at[k, pl.ds(h * tall, tall)], leg_sem.at[k, h]

        def col_ref(dz, core, h):
            k = zs(dz) * 2 + core
            return C.at[k, pl.ds(*parts[h])], far_sem.at[k, h]

        def col_block(dz):
            k = zs(dz) * 2 + c
            return C.at[k], block_sem.at[k]

        def leg(ref, sem, **where):
            start(ref, ref, row_sent, sem, **where)

        def hop(ref, sem, **where):
            start(ref, ref, col_sent, sem, **where)

        def twin(ref, dz):
            hop(ref, twin_sem.at[0 if dz in EARLY else 1], c=c1)

        for h in chunks:
            for dz in (2, -2):
                hop(*col_ref(0, c, h), z=zs(dz))
        for h in chunks:
            for dz in (1, -1):
                hop(col_ref(0, c, h)[0], col_block(0)[1], z=zs(dz))
        for h, v in pairs:
            for d in (2, 1, -1):
                leg(*row_ref(0, 0, h), **xs(d))
                leg(*row_ref(0, 0, v), y=ys(d))
        twin(col_block(0)[0], 0)
        for h, v in pairs:
            for d in (2, 1, -1):
                leg(row_ref(0, 0, v)[0], rest_sem, **xs(d))
                leg(row_ref(0, 0, h)[0], rest_sem, y=ys(d))

        for step in chunks:
            h, v = pairs[step]
            for d in (1, -1, 2):
                item = row_ref(0, d, h)
                arrived(*item)
                for e in (2, 1, -1):
                    leg(item[0], rest_sem, y=ys(e))
                item = row_ref(d, 0, v)
                arrived(*item)
                for e in (2, 1, -1):
                    leg(item[0], rest_sem, **xs(e))
            for sign in (1, -1):
                item = col_ref(-2 * sign, c, step)
                arrived(*item)
                if (step % 2 == 0) == (sign > 0):
                    hop(item[0], col_block(-2 * sign)[1], z=zs(2 * sign))
                hop(item[0], col_block(-2 * sign)[1], z=zs(sign))
                twin(item[0], -2)
        for dz in (-1, 1) + LATE:
            item = col_block(dz)
            arrived(*item)
            twin(item[0], dz)
        extra()
        arrived(R.at[pl.ds(0, 12)], rest_sem)
        arrived(C.at[pl.ds(0, len(EARLY))], twin_sem.at[0])
        ready(EARLY)
        arrived(C.at[pl.ds(0, len(LATE))], twin_sem.at[1])

    def sent(R, C, sems):
        left_here(R.at[pl.ds(0, N - 1)], sems[-2])
        left_here(C.at[pl.ds(0, N - 1)], sems[-1])

    def give_stat():
        send(R1.at[gj], s_new, swap_sem.at[1], swaps, a=a1, c=c1)

    def strips(R, k):
        return split(jnp.concatenate([R[2 * k], R[2 * k + 1]], axis=1))

    def columns(C, k):
        rows = jnp.concatenate([C[2 * k, :B], C[2 * k + 1, :B]], axis=0)
        return jnp.concatenate(split(rows), axis=1)

    total = []

    def square(steps):
        for dz in steps:
            k = zs(dz)
            CB[k] = columns(C1, k)
            total.append(jnp.dot(
                jnp.concatenate(strips(R1, k), axis=0), CB[k], preferred_element_type=jnp.float32
            ))

    exchange(R1, C1, sems1, B, give_stat, square)
    square(LATE)
    squares = jnp.zeros((PAD, B), jnp.float32)
    for k in range(N):
        block = R1[k]
        squares = squares + jnp.sum((block * block).reshape(B // PAD, PAD, B), axis=0)
    mid = fold4(sum(total[1:], total[0]))
    R2[gj] = mid
    C2[gi, :B] = mid
    C2[gi, B:] = squares

    def keep_stat():
        @pl.when(swaps)
        def _():
            arrived(s_new, swap_sem.at[1])
            s_out[...] = s_new[...]

        @pl.when(a == c)
        def _():
            s_out[...] = R1[gj]

    half = B // 2
    wide = [[], []]

    def powers(steps, halves):
        for part in halves:
            for dz in steps:
                k = zs(dz)
                both = jnp.concatenate([CB[k], columns(C2, k)], axis=1)
                hi, lo = strips(R2, k)
                cut = slice(part * half, part * half + half)
                wide[part].append(jnp.dot(
                    jnp.concatenate([hi[cut], lo[cut]], axis=0), both, preferred_element_type=jnp.float32
                ))

    exchange(R2, C2, sems2, B + PAD, keep_stat, lambda steps: powers(steps, (0, 1)))

    squares = jnp.zeros((PAD, B), jnp.float32)
    for k in range(N):
        squares = squares + C2[k, B:]
    whole = jnp.sum(squares, keepdims=True)
    inv = 1.0 / (2.0 * jnp.sqrt(whole / float(N * B)))
    rows = lax.broadcasted_iota(jnp.int32, (half, B), 0) + gi * B
    cols = lax.broadcasted_iota(jnp.int32, (half, B), 1) + gj * B

    def fold2(full):
        return (full[:half, :B] + full[half:, :B]) + (full[:half, B:] + full[half:, B:])

    for part in (0, 1):
        powers(LATE, (part,))
        full = sum(wide[part][1:], wide[part][0])
        cube = fold2(full[:, : 2 * B])
        quad = fold2(full[:, 2 * B:])
        cut = pl.ds(part * half, half)
        eye = jnp.where(rows + part * half == cols, A0, 0.0)
        tail = A2 * R2[gj, cut] + inv * (A3 * cube + inv * (A4 * quad))
        r_own[cut] = eye + inv * (A1 * R1[gj, cut] + inv * tail)
        send(r_own.at[cut], r_new.at[cut], swap_sem.at[2 + part], swaps, a=a1, c=c1)

    @pl.when(swaps)
    def _():
        for part in (0, 1):
            cut = pl.ds(part * half, half)
            arrived(r_new.at[cut], swap_sem.at[2 + part])
            r_out[cut] = r_new[cut]

    @pl.when(a == c)
    def _():
        r_out[...] = r_own[...]

    left_here(R1.at[pl.ds(0, 11), pl.ds(0, 2 * KP)], piece_sem)
    sent(R1, C1, sems1)
    sent(R2, C2, sems2)
    for copy, cond in sends:
        pl.when(cond)(copy.wait_send)


def local(gradient, stat_old):
    f32 = jnp.float32
    dma = pltpu.SemaphoreType.DMA
    tile = pltpu.VMEM((B, B), f32)
    pieces = pltpu.VMEM((N, KP, B), f32)
    strip = pltpu.VMEM((N, B, B), f32)
    gather_sems = [dma((N, RH)), dma, dma((N, CH)), dma((N,)), dma((2,)), dma, dma]
    return pl.pallas_call(
        kernel,
        out_shape=(pltpu.VMEM((B, B), f32), pltpu.VMEM((B, B), f32)),
        in_specs=[pl.BlockSpec(memory_space=pl.ANY)] * 2,
        out_specs=[pl.BlockSpec(memory_space=pltpu.VMEM)] * 2,
        scratch_shapes=[
            tile, pltpu.VMEM((KP, B), f32), pieces, pieces,
            strip, strip, strip, pltpu.VMEM((N, B + PAD, B), f32),
            pltpu.VMEM((N // 2, 2 * B, 2 * B), jnp.bfloat16),
            tile, tile, tile, tile,
            dma((2,)), dma, dma((2,)), dma, dma((2,)), dma((4,)), dma, dma((16,)),
            *gather_sems, *gather_sems,
        ],
        compiler_params=pltpu.CompilerParams(collective_id=0, has_side_effects=True),
    )(gradient.T, stat_old)


def solution(mesh):
    torus = Mesh(mesh.devices.reshape(8, 2, 4, 2, 2), ("z", "a", "y", "b", "c"))
    return jax.shard_map(
        local, mesh=torus, in_specs=(P(GX, GY), P(GX, GY)),
        out_specs=(P(GX, GY), P(GX, GY)), check_vma=False,
    )
```

```python
import jax
import jax.numpy as jnp
from jax import lax
from jax.experimental import pallas as pl
from jax.experimental.pallas import tpu as pltpu
from jax.sharding import Mesh
from jax.sharding import PartitionSpec as P

MESH = pl.DeviceIdType.MESH
GX = ("z", "a")
GY = ("y", "b", "c")
B = 128
CH = 2
RH = 4
EARLY = (0, -1, 1, -2, 2)
LATE = (-3, 3, 4)
PAD = 8
KP = 32
N = 16

A0, A1, A2, A3, A4 = 2.25, -2.4375, 1.6875, -0.5625, 0.0625


def split(x):
    hi = x.astype(jnp.bfloat16)
    lo = (x - hi.astype(jnp.float32)).astype(jnp.bfloat16)
    return hi, lo


def fold4(full):
    return (full[:B, :B] + full[B:, :B]) + (full[:B, B:] + full[B:, B:])


def kernel(
    g_hbm, a_hbm, s_out, r_out,
    a_in, gt, GI, GJ, R1, C1, R2, C2, CB, a_new, s_new, r_own, r_new,
    in_sem, gi_sem, gj_sem, gs_sem, down_sem, swap_sem, piece_sem, send_sem, *gather_sems,
):
    z, a = lax.axis_index("z"), lax.axis_index("a")
    y, b, c = lax.axis_index("y"), lax.axis_index("b"), lax.axis_index("c")
    a1, b1, c1 = 1 - a, 1 - b, 1 - c
    x = 2 * b + a
    gi = z * 2 + c
    gj = y * 4 + x
    own = c * 8 + y * 2 + b
    home = z == 2 * y + b
    swaps = a != c

    sems1, sems2 = gather_sems[:7], gather_sems[7:]
    load_g = pltpu.make_async_copy(g_hbm, gt, in_sem.at[0])
    load_a = pltpu.make_async_copy(a_hbm, a_in, in_sem.at[1])
    load_g.start()
    load_a.start()

    barrier = pltpu.get_barrier_semaphore()

    def greet(**where):
        pl.semaphore_signal(barrier, inc=1, device_id=where, device_id_type=MESH)

    def zs(dz):
        return lax.rem(z + dz + 8, 8)

    def ys(dy):
        return lax.rem(y + dy + 4, 4)

    def xs(dx):
        to = lax.rem(x + dx + 4, 4)
        return {"b": to // 2, "a": lax.rem(to, 2)}

    def place(slot):
        return {"y": lax.rem(slot // 2, 4), "b": lax.rem(slot, 2), "c": slot // 8}

    @pl.when(c == 0)
    def _():
        for t in range(1, N):
            greet(z=2 * y + b, **place(lax.rem(own + t, N)))

        @pl.when(jnp.logical_not(home))
        def _():
            greet(z=2 * y + b)

    for t in range(1, N):
        greet(a=c, **place(lax.rem(own + t, N)))

    @pl.when(swaps)
    def _():
        greet(a=c)

    @pl.when(swaps)
    def _():
        greet(a=a1, c=c1)

    @pl.when(c == 1)
    def _():
        greet(c=0)

    for dz in (2, -2, 1, -1):
        greet(z=zs(dz))
    for d in (2, 1, -1):
        greet(y=ys(d))
        greet(**xs(d))
    greet(c=c1)
    alike = jnp.where(a == c, 1, 0)
    at_home = jnp.where(home, 1, 0)
    expected = 36 - 2 * alike + (1 - c) - (1 - c) * at_home

    load_g.wait()
    pl.semaphore_wait(barrier, expected)

    sends = []

    def start(src, dst, ssem, rsem, **where):
        copy = pltpu.make_async_remote_copy(
            src_ref=src, dst_ref=dst, send_sem=ssem, recv_sem=rsem,
            device_id=where, device_id_type=MESH,
        )
        copy.start()

    def send(src, dst, rsem, cond, **where):
        copy = pltpu.make_async_remote_copy(
            src_ref=src, dst_ref=dst, send_sem=send_sem.at[len(sends)], recv_sem=rsem,
            device_id=where, device_id_type=MESH,
        )
        pl.when(cond)(copy.start)
        sends.append((copy, cond))

    def left_here(ref, ssem):
        pltpu.make_async_remote_copy(
            src_ref=ref, dst_ref=ref, send_sem=ssem, recv_sem=gs_sem,
            device_id={"c": c1}, device_id_type=MESH,
        ).wait_send()

    def arrived(ref, rsem):
        pltpu.make_async_remote_copy(
            src_ref=ref, dst_ref=ref, send_sem=gs_sem, recv_sem=rsem,
            device_id={"c": c1}, device_id_type=MESH,
        ).wait_recv()

    col_y, col_b = z // 2, lax.rem(z, 2)
    for dz in (4, 3, 5, 2, 6, 1, 7):
        start(gt, GJ.at[own], piece_sem, gj_sem.at[c], z=zs(dz), y=col_y, b=col_b, c=0)
    away = jnp.logical_not(jnp.logical_and(home, c == 0))
    send(gt, GJ.at[own], gj_sem.at[c], away, y=col_y, b=col_b, c=0)
    for dx in (2, 1, -1, 0):
        for dy in (2, 1, -1, 0):
            if dx or dy:
                to = xs(dx)
                start(gt, GI.at[own], piece_sem, gi_sem, y=ys(dy), b=to["b"], a=to["a"], c=a)
    send(gt, GI.at[own], gi_sem, swaps, c=a)

    load_a.wait()
    send(a_in, a_new, swap_sem.at[0], swaps, a=a1, c=c1)

    @pl.when(a == c)
    def _():
        GI[own] = gt[...]
        a_new[...] = a_in[...]

    @pl.when(jnp.logical_and(home, c == 0))
    def _():
        GJ[own] = gt[...]

    lower = GJ.at[pl.ds(0, 8)]
    upper = GJ.at[pl.ds(8, 8)]

    @pl.when(c == 0)
    def _():
        @pl.when(home)
        def _():
            arrived(GJ.at[pl.ds(0, 7)], gj_sem.at[0])

        @pl.when(jnp.logical_not(home))
        def _():
            arrived(lower, gj_sem.at[0])

    send(lower, lower, down_sem.at[0], c == 0, c=c1)

    @pl.when(c == 0)
    def _():
        arrived(upper, gj_sem.at[1])

    send(upper, upper, down_sem.at[1], c == 0, c=c1)

    @pl.when(a == c)
    def _():
        arrived(GI.at[pl.ds(0, N - 1)], gi_sem)

    @pl.when(swaps)
    def _():
        arrived(GI, gi_sem)
        arrived(a_new, swap_sem.at[0])

    @pl.when(c == 1)
    def _():
        arrived(lower, down_sem.at[0])
        arrived(upper, down_sem.at[1])

    left = jnp.transpose(GI[...].reshape(N * KP, B))
    right = GJ[...].reshape(N * KP, B)
    lh, ll = split(left)
    rh, rl = split(right)
    full = jnp.dot(
        jnp.concatenate([lh, ll], axis=0), jnp.concatenate([rh, rl], axis=1),
        preferred_element_type=jnp.float32,
    )
    stat = 0.9 * a_new[...] + fold4(full) / float(N * KP)
    R1[gj] = stat
    C1[gi] = stat

    def exchange(R, C, sems, rows, extra, ready):
        width = B // CH
        parts = [(h * width, width) for h in range(CH)]
        parts[-1] = (B - width, width + rows - B)
        chunks = range(CH)
        tall = B // RH
        pairs = [(h, h + RH // 2) for h in range(RH // 2)]
        leg_sem, rest_sem, far_sem, block_sem, twin_sem, row_sent, col_sent = sems

        def row_ref(dy, dx, h):
            k = ys(dy) * 4 + lax.rem(x + dx + 4, 4)
            return R.at[k, pl.ds(h * tall, tall)]

        def leg_of(d, h):
            return leg_sem.at[d % 4 - 1, h]

        def col_ref(dz, h):
            return C.at[zs(dz) * 2 + c, pl.ds(*parts[h])]

        def far_of(dz, h):
            return far_sem.at[0 if dz > 0 else 1, h]

        def block_of(dz):
            return block_sem.at[(1, -1, 3, -3, 4).index(dz)]

        def leg(ref, sem, **where):
            start(ref, ref, row_sent, sem, **where)

        def hop(ref, sem, **where):
            start(ref, ref, col_sent, sem, **where)

        def twin(ref, dz):
            hop(ref, twin_sem.at[0 if dz in EARLY else 1], c=c1)

        for h in chunks:
            for dz in (2, -2):
                hop(col_ref(0, h), far_of(-dz, h), z=zs(dz))
        for h in chunks:
            for dz in (1, -1):
                hop(col_ref(0, h), block_of(-dz), z=zs(dz))
        for h, v in pairs:
            for d in (2, 1, -1):
                leg(row_ref(0, 0, h), leg_of(-d, h), **xs(d))
                leg(row_ref(0, 0, v), leg_of(-d, v), y=ys(d))
        twin(C.at[gi], 0)
        for h, v in pairs:
            for d in (2, 1, -1):
                leg(row_ref(0, 0, v), rest_sem, **xs(d))
                leg(row_ref(0, 0, h), rest_sem, y=ys(d))

        for step in chunks:
            h, v = pairs[step]
            for d in (1, -1, 2):
                item = row_ref(0, d, h)
                arrived(item, leg_of(d, h))
                for e in (2, 1, -1):
                    leg(item, rest_sem, y=ys(e))
                item = row_ref(d, 0, v)
                arrived(item, leg_of(d, v))
                for e in (2, 1, -1):
                    leg(item, rest_sem, **xs(e))
            for sign in (1, -1):
                item = col_ref(-2 * sign, step)
                arrived(item, far_of(-2 * sign, step))
                if (step % 2 == 0) == (sign > 0):
                    hop(item, block_of(4), z=zs(2 * sign))
                hop(item, block_of(-3 * sign), z=zs(sign))
                twin(item, -2)
        for dz in (-1, 1) + LATE:
            item = C.at[zs(dz) * 2 + c]
            arrived(item, block_of(dz))
            twin(item, dz)
        extra()
        arrived(R.at[pl.ds(0, 12)], rest_sem)
        arrived(C.at[pl.ds(0, len(EARLY))], twin_sem.at[0])
        ready(EARLY)
        arrived(C.at[pl.ds(0, len(LATE))], twin_sem.at[1])

    def sent(R, C, sems):
        left_here(R.at[pl.ds(0, N - 1)], sems[-2])
        left_here(C.at[pl.ds(0, N - 1)], sems[-1])

    def give_stat():
        send(R1.at[gj], s_new, swap_sem.at[1], swaps, a=a1, c=c1)

    def strips(R, k):
        return split(jnp.concatenate([R[2 * k], R[2 * k + 1]], axis=1))

    def columns(C, k):
        rows = jnp.concatenate([C[2 * k, :B], C[2 * k + 1, :B]], axis=0)
        return jnp.concatenate(split(rows), axis=1)

    total = []

    def square(steps):
        for dz in steps:
            k = zs(dz)
            CB[k] = columns(C1, k)
            total.append(jnp.dot(
                jnp.concatenate(strips(R1, k), axis=0), CB[k], preferred_element_type=jnp.float32
            ))

    exchange(R1, C1, sems1, B, give_stat, square)
    square(LATE)
    squares = jnp.zeros((PAD, B), jnp.float32)
    for k in range(N):
        block = R1[k]
        squares = squares + jnp.sum((block * block).reshape(B // PAD, PAD, B), axis=0)
    mid = fold4(sum(total[1:], total[0]))
    R2[gj] = mid
    C2[gi, :B] = mid
    C2[gi, B:] = squares

    def keep_stat():
        @pl.when(swaps)
        def _():
            arrived(s_new, swap_sem.at[1])
            s_out[...] = s_new[...]

        @pl.when(a == c)
        def _():
            s_out[...] = R1[gj]

    half = B // 2
    wide = [[], []]

    def powers(steps, halves):
        for part in halves:
            for dz in steps:
                k = zs(dz)
                both = jnp.concatenate([CB[k], columns(C2, k)], axis=1)
                hi, lo = strips(R2, k)
                cut = slice(part * half, part * half + half)
                wide[part].append(jnp.dot(
                    jnp.concatenate([hi[cut], lo[cut]], axis=0), both, preferred_element_type=jnp.float32
                ))

    exchange(R2, C2, sems2, B + PAD, keep_stat, lambda steps: powers(steps, (0, 1)))

    squares = jnp.zeros((PAD, B), jnp.float32)
    for k in range(N):
        squares = squares + C2[k, B:]
    whole = jnp.sum(squares, keepdims=True)
    inv = 1.0 / (2.0 * jnp.sqrt(whole / float(N * B)))
    rows = lax.broadcasted_iota(jnp.int32, (half, B), 0) + gi * B
    cols = lax.broadcasted_iota(jnp.int32, (half, B), 1) + gj * B

    def fold2(full):
        return (full[:half, :B] + full[half:, :B]) + (full[:half, B:] + full[half:, B:])

    for part in (0, 1):
        powers(LATE, (part,))
        full = sum(wide[part][1:], wide[part][0])
        cube = fold2(full[:, : 2 * B])
        quad = fold2(full[:, 2 * B:])
        cut = pl.ds(part * half, half)
        eye = jnp.where(rows + part * half == cols, A0, 0.0)
        tail = A2 * R2[gj, cut] + inv * (A3 * cube + inv * (A4 * quad))
        r_own[cut] = eye + inv * (A1 * R1[gj, cut] + inv * tail)
        send(r_own.at[cut], r_new.at[cut], swap_sem.at[2 + part], swaps, a=a1, c=c1)

    @pl.when(swaps)
    def _():
        for part in (0, 1):
            cut = pl.ds(part * half, half)
            arrived(r_new.at[cut], swap_sem.at[2 + part])
            r_out[cut] = r_new[cut]

    @pl.when(a == c)
    def _():
        r_out[...] = r_own[...]

    left_here(R1.at[pl.ds(0, 11), pl.ds(0, 2 * KP)], piece_sem)
    sent(R1, C1, sems1)
    sent(R2, C2, sems2)
    for copy, cond in sends:
        pl.when(cond)(copy.wait_send)


def local(gradient, stat_old):
    f32 = jnp.float32
    dma = pltpu.SemaphoreType.DMA
    tile = pltpu.VMEM((B, B), f32)
    pieces = pltpu.VMEM((N, KP, B), f32)
    strip = pltpu.VMEM((N, B, B), f32)
    gather_sems = [dma((3, RH)), dma, dma((2, CH)), dma((5,)), dma((2,)), dma, dma]
    return pl.pallas_call(
        kernel,
        out_shape=(pltpu.VMEM((B, B), f32), pltpu.VMEM((B, B), f32)),
        in_specs=[pl.BlockSpec(memory_space=pl.ANY)] * 2,
        out_specs=[pl.BlockSpec(memory_space=pltpu.VMEM)] * 2,
        scratch_shapes=[
            tile, pltpu.VMEM((KP, B), f32), pieces, pieces,
            strip, strip, strip, pltpu.VMEM((N, B + PAD, B), f32),
            pltpu.VMEM((N // 2, 2 * B, 2 * B), jnp.bfloat16),
            tile, tile, tile, tile,
            dma((2,)), dma, dma((2,)), dma, dma((2,)), dma((4,)), dma, dma((9,)),
            *gather_sems, *gather_sems,
        ],
        compiler_params=pltpu.CompilerParams(collective_id=0, has_side_effects=True),
    )(gradient.T, stat_old)


def solution(mesh):
    torus = Mesh(mesh.devices.reshape(8, 2, 4, 2, 2), ("z", "a", "y", "b", "c"))
    return jax.shard_map(
        local, mesh=torus, in_specs=(P(GX, GY), P(GX, GY)),
        out_specs=(P(GX, GY), P(GX, GY)), check_vma=False,
    )
```

```python
import jax
import jax.numpy as jnp
from jax import lax
from jax.experimental import pallas as pl
from jax.experimental.pallas import tpu as pltpu
from jax.sharding import Mesh
from jax.sharding import PartitionSpec as P

MESH = pl.DeviceIdType.MESH
GX = ("z", "a")
GY = ("y", "b", "c")
B = 128
CH = 2
RH = 4
EARLY = (0, -1, 1, -2, 2)
LATE = (-3, 3, 4)
PAD = 8
KP = 32
N = 16

A0, A1, A2, A3, A4 = 2.25, -2.4375, 1.6875, -0.5625, 0.0625


def split(x):
    hi = x.astype(jnp.bfloat16)
    lo = (x - hi.astype(jnp.float32)).astype(jnp.bfloat16)
    return hi, lo


def fold4(full):
    return (full[:B, :B] + full[B:, :B]) + (full[:B, B:] + full[B:, B:])


def kernel(
    g_hbm, a_hbm, both_out,
    a_in, gt, GI, GJ, R1, C1, R2, C2, CB, a_new, s_new, r_own, r_new,
    in_sem, gi_sem, gj_sem, gs_sem, down_sem, swap_sem, piece_sem, send_sem, *gather_sems,
):
    z, a = lax.axis_index("z"), lax.axis_index("a")
    y, b, c = lax.axis_index("y"), lax.axis_index("b"), lax.axis_index("c")
    a1, b1, c1 = 1 - a, 1 - b, 1 - c
    x = 2 * b + a
    gi = z * 2 + c
    gj = y * 4 + x
    own = c * 8 + y * 2 + b
    home = z == 2 * y + b
    swaps = a != c

    sems1, sems2 = gather_sems[:7], gather_sems[7:]
    s_out, r_out = both_out.at[0], both_out.at[1]
    load_g = pltpu.make_async_copy(g_hbm, gt, in_sem.at[0])
    load_a = pltpu.make_async_copy(a_hbm, a_in, in_sem.at[1])
    load_g.start()
    load_a.start()

    barrier = pltpu.get_barrier_semaphore()

    def greet(**where):
        pl.semaphore_signal(barrier, inc=1, device_id=where, device_id_type=MESH)

    def zs(dz):
        return lax.rem(z + dz + 8, 8)

    def ys(dy):
        return lax.rem(y + dy + 4, 4)

    def xs(dx):
        to = lax.rem(x + dx + 4, 4)
        return {"b": to // 2, "a": lax.rem(to, 2)}

    others = [
        {"y": ys(dy), "b": pb, "c": pc}
        for dy in (2, 1, -1, 0) for pb in (b1, b) for pc in (c1, c)
    ][:-1]

    @pl.when(c == 0)
    def _():
        for where in others:
            greet(z=2 * y + b, **where)

        @pl.when(jnp.logical_not(home))
        def _():
            greet(z=2 * y + b)

    for where in others:
        greet(a=c, **where)

    @pl.when(swaps)
    def _():
        greet(a=c)

    @pl.when(swaps)
    def _():
        greet(a=a1, c=c1)

    @pl.when(c == 1)
    def _():
        greet(c=0)

    for dz in (2, -2, 1, -1):
        greet(z=zs(dz))
    for d in (2, 1, -1):
        greet(y=ys(d))
        greet(**xs(d))
    greet(c=c1)
    alike = jnp.where(a == c, 1, 0)
    at_home = jnp.where(home, 1, 0)
    expected = 36 - 2 * alike + (1 - c) - (1 - c) * at_home

    load_g.wait()
    pl.semaphore_wait(barrier, expected)

    sends = []

    def start(src, dst, ssem, rsem, **where):
        copy = pltpu.make_async_remote_copy(
            src_ref=src, dst_ref=dst, send_sem=ssem, recv_sem=rsem,
            device_id=where, device_id_type=MESH,
        )
        copy.start()

    def send(src, dst, rsem, cond, **where):
        copy = pltpu.make_async_remote_copy(
            src_ref=src, dst_ref=dst, send_sem=send_sem.at[len(sends)], recv_sem=rsem,
            device_id=where, device_id_type=MESH,
        )
        pl.when(cond)(copy.start)
        sends.append((copy, cond))

    def left_here(ref, ssem):
        pltpu.make_async_remote_copy(
            src_ref=ref, dst_ref=ref, send_sem=ssem, recv_sem=gs_sem,
            device_id={"c": c1}, device_id_type=MESH,
        ).wait_send()

    def arrived(ref, rsem):
        pltpu.make_async_remote_copy(
            src_ref=ref, dst_ref=ref, send_sem=gs_sem, recv_sem=rsem,
            device_id={"c": c1}, device_id_type=MESH,
        ).wait_recv()

    col_y, col_b = z // 2, lax.rem(z, 2)
    for dz in (4, 3, 5, 2, 6, 1, 7):
        start(gt, GJ.at[own], piece_sem, gj_sem.at[c], z=zs(dz), y=col_y, b=col_b, c=0)
    away = jnp.logical_not(jnp.logical_and(home, c == 0))
    send(gt, GJ.at[own], gj_sem.at[c], away, y=col_y, b=col_b, c=0)
    for dx in (2, 1, -1, 0):
        for dy in (2, 1, -1, 0):
            if dx or dy:
                to = xs(dx)
                start(gt, GI.at[own], piece_sem, gi_sem, y=ys(dy), b=to["b"], a=to["a"], c=a)
    send(gt, GI.at[own], gi_sem, swaps, c=a)

    load_a.wait()
    send(a_in, a_new, swap_sem.at[0], swaps, a=a1, c=c1)

    @pl.when(a == c)
    def _():
        GI[own] = gt[...]
        a_new[...] = a_in[...]

    @pl.when(jnp.logical_and(home, c == 0))
    def _():
        GJ[own] = gt[...]

    lower = GJ.at[pl.ds(0, 8)]
    upper = GJ.at[pl.ds(8, 8)]

    @pl.when(c == 0)
    def _():
        @pl.when(home)
        def _():
            arrived(GJ.at[pl.ds(0, 7)], gj_sem.at[0])

        @pl.when(jnp.logical_not(home))
        def _():
            arrived(lower, gj_sem.at[0])

    send(lower, lower, down_sem.at[0], c == 0, c=c1)

    @pl.when(c == 0)
    def _():
        arrived(upper, gj_sem.at[1])

    send(upper, upper, down_sem.at[1], c == 0, c=c1)

    @pl.when(a == c)
    def _():
        arrived(GI.at[pl.ds(0, N - 1)], gi_sem)

    @pl.when(swaps)
    def _():
        arrived(GI, gi_sem)
        arrived(a_new, swap_sem.at[0])

    @pl.when(c == 1)
    def _():
        arrived(lower, down_sem.at[0])
        arrived(upper, down_sem.at[1])

    left = jnp.transpose(GI[...].reshape(N * KP, B))
    right = GJ[...].reshape(N * KP, B)
    lh, ll = split(left)
    rh, rl = split(right)
    full = jnp.dot(
        jnp.concatenate([lh, ll], axis=0), jnp.concatenate([rh, rl], axis=1),
        preferred_element_type=jnp.float32,
    )
    stat = 0.9 * a_new[...] + fold4(full) / float(N * KP)
    R1[gj] = stat
    C1[gi] = stat

    def exchange(R, C, sems, rows, extra, ready):
        width = B // CH
        parts = [(h * width, width) for h in range(CH)]
        parts[-1] = (B - width, width + rows - B)
        chunks = range(CH)
        tall = B // RH
        pairs = [(h, h + RH // 2) for h in range(RH // 2)]
        leg_sem, rest_sem, far_sem, block_sem, twin_sem, row_sent, col_sent = sems

        def row_ref(dy, dx, h):
            k = ys(dy) * 4 + lax.rem(x + dx + 4, 4)
            return R.at[k, pl.ds(h * tall, tall)]

        def leg_of(d, h):
            return leg_sem.at[d % 4 - 1, h]

        def col_ref(dz, h):
            return C.at[zs(dz) * 2 + c, pl.ds(*parts[h])]

        def far_of(dz, h):
            return far_sem.at[0 if dz > 0 else 1, h]

        def block_of(dz):
            return block_sem.at[(1, -1, 3, -3, 4).index(dz)]

        def leg(ref, sem, **where):
            start(ref, ref, row_sent, sem, **where)

        def hop(ref, sem, **where):
            start(ref, ref, col_sent, sem, **where)

        def twin(ref, dz):
            hop(ref, twin_sem.at[0 if dz in EARLY else 1], c=c1)

        for h in chunks:
            for dz in (2, -2):
                hop(col_ref(0, h), far_of(-dz, h), z=zs(dz))
        for h in chunks:
            for dz in (1, -1):
                hop(col_ref(0, h), block_of(-dz), z=zs(dz))
        for h, v in pairs:
            for d in (2, 1, -1):
                leg(row_ref(0, 0, h), leg_of(-d, h), **xs(d))
                leg(row_ref(0, 0, v), leg_of(-d, v), y=ys(d))
        twin(C.at[gi], 0)
        for h, v in pairs:
            for d in (2, 1, -1):
                leg(row_ref(0, 0, v), rest_sem, **xs(d))
                leg(row_ref(0, 0, h), rest_sem, y=ys(d))

        for step in chunks:
            h, v = pairs[step]
            for d in (1, -1, 2):
                item = row_ref(0, d, h)
                arrived(item, leg_of(d, h))
                for e in (2, 1, -1):
                    leg(item, rest_sem, y=ys(e))
                item = row_ref(d, 0, v)
                arrived(item, leg_of(d, v))
                for e in (2, 1, -1):
                    leg(item, rest_sem, **xs(e))
            for sign in (1, -1):
                item = col_ref(-2 * sign, step)
                arrived(item, far_of(-2 * sign, step))
                if (step % 2 == 0) == (sign > 0):
                    hop(item, block_of(4), z=zs(2 * sign))
                hop(item, block_of(-3 * sign), z=zs(sign))
                twin(item, -2)
        for dz in (-1, 1) + LATE:
            item = C.at[zs(dz) * 2 + c]
            arrived(item, block_of(dz))
            twin(item, dz)
        extra()
        arrived(R.at[pl.ds(0, 12)], rest_sem)
        arrived(C.at[pl.ds(0, len(EARLY))], twin_sem.at[0])
        ready(EARLY)
        arrived(C.at[pl.ds(0, len(LATE))], twin_sem.at[1])

    def sent(R, C, sems):
        left_here(R.at[pl.ds(0, N - 1)], sems[-2])
        left_here(C.at[pl.ds(0, N - 1)], sems[-1])

    def give_stat():
        send(R1.at[gj], s_new, swap_sem.at[1], swaps, a=a1, c=c1)

    def strips(R, k):
        return split(jnp.concatenate([R[2 * k], R[2 * k + 1]], axis=1))

    def columns(C, k):
        rows = jnp.concatenate([C[2 * k, :B], C[2 * k + 1, :B]], axis=0)
        return jnp.concatenate(split(rows), axis=1)

    total = []
    norms = []

    def square(steps):
        if not norms:
            norms.append(jnp.zeros((PAD, B), jnp.float32))
            for k in range(N):
                block = R1[k]
                norms[0] = norms[0] + jnp.sum((block * block).reshape(B // PAD, PAD, B), axis=0)
        for dz in steps:
            k = zs(dz)
            CB[k] = columns(C1, k)
            total.append(jnp.dot(
                jnp.concatenate(strips(R1, k), axis=0), CB[k], preferred_element_type=jnp.float32
            ))

    exchange(R1, C1, sems1, B, give_stat, square)
    square(LATE)
    mid = fold4(sum(total[1:], total[0]))
    R2[gj] = mid
    C2[gi, :B] = mid
    C2[gi, B:] = norms[0]

    def keep_stat():
        @pl.when(swaps)
        def _():
            arrived(s_new, swap_sem.at[1])
            s_out[...] = s_new[...]

        @pl.when(a == c)
        def _():
            s_out[...] = R1[gj]

    half = B // 2
    wide = [[], []]

    def powers(steps, halves):
        for part in halves:
            for dz in steps:
                k = zs(dz)
                both = jnp.concatenate([CB[k], columns(C2, k)], axis=1)
                hi, lo = strips(R2, k)
                cut = slice(part * half, part * half + half)
                wide[part].append(jnp.dot(
                    jnp.concatenate([hi[cut], lo[cut]], axis=0), both, preferred_element_type=jnp.float32
                ))

    exchange(R2, C2, sems2, B + PAD, keep_stat, lambda steps: powers(steps, (0, 1)))

    squares = jnp.zeros((PAD, B), jnp.float32)
    for k in range(N):
        squares = squares + C2[k, B:]
    whole = jnp.sum(squares, keepdims=True)
    inv = 1.0 / (2.0 * jnp.sqrt(whole / float(N * B)))
    rows = lax.broadcasted_iota(jnp.int32, (half, B), 0) + gi * B
    cols = lax.broadcasted_iota(jnp.int32, (half, B), 1) + gj * B

    def fold2(full):
        return (full[:half, :B] + full[half:, :B]) + (full[:half, B:] + full[half:, B:])

    for part in (0, 1):
        powers(LATE, (part,))
        full = sum(wide[part][1:], wide[part][0])
        cube = fold2(full[:, : 2 * B])
        quad = fold2(full[:, 2 * B:])
        cut = pl.ds(part * half, half)
        eye = jnp.where(rows + part * half == cols, A0, 0.0)
        tail = A2 * R2[gj, cut] + inv * (A3 * cube + inv * (A4 * quad))
        r_own[cut] = eye + inv * (A1 * R1[gj, cut] + inv * tail)
        send(r_own.at[cut], r_new.at[cut], swap_sem.at[2 + part], swaps, a=a1, c=c1)

    @pl.when(swaps)
    def _():
        for part in (0, 1):
            cut = pl.ds(part * half, half)
            arrived(r_new.at[cut], swap_sem.at[2 + part])
            r_out[cut] = r_new[cut]

    @pl.when(a == c)
    def _():
        r_out[...] = r_own[...]

    left_here(R1.at[pl.ds(0, 11), pl.ds(0, 2 * KP)], piece_sem)
    sent(R1, C1, sems1)
    sent(R2, C2, sems2)
    for copy, cond in sends:
        pl.when(cond)(copy.wait_send)


def local(gradient, stat_old):
    f32 = jnp.float32
    dma = pltpu.SemaphoreType.DMA
    tile = pltpu.VMEM((B, B), f32)
    pieces = pltpu.VMEM((N, KP, B), f32)
    strip = pltpu.VMEM((N, B, B), f32)
    gather_sems = [dma((3, RH)), dma, dma((2, CH)), dma((5,)), dma((2,)), dma, dma]
    both = pl.pallas_call(
        kernel,
        out_shape=pltpu.VMEM((2, B, B), f32),
        in_specs=[pl.BlockSpec(memory_space=pl.ANY)] * 2,
        out_specs=pl.BlockSpec(memory_space=pltpu.VMEM),
        scratch_shapes=[
            tile, pltpu.VMEM((KP, B), f32), pieces, pieces,
            strip, strip, strip, pltpu.VMEM((N, B + PAD, B), f32),
            pltpu.VMEM((N // 2, 2 * B, 2 * B), jnp.bfloat16),
            tile, tile, tile, tile,
            dma((2,)), dma, dma((2,)), dma, dma((2,)), dma((4,)), dma, dma((9,)),
            *gather_sems, *gather_sems,
        ],
        compiler_params=pltpu.CompilerParams(collective_id=0, has_side_effects=True),
    )(gradient.T, stat_old)
    return both[0], both[1]


def solution(mesh):
    torus = Mesh(mesh.devices.reshape(8, 2, 4, 2, 2), ("z", "a", "y", "b", "c"))
    return jax.shard_map(
        local, mesh=torus, in_specs=(P(GX, GY), P(GX, GY)),
        out_specs=(P(GX, GY), P(GX, GY)), check_vma=False,
    )
```

```python
import jax
import jax.numpy as jnp
from jax import lax
from jax.experimental import pallas as pl
from jax.experimental.pallas import tpu as pltpu
from jax.sharding import Mesh
from jax.sharding import PartitionSpec as P

MESH = pl.DeviceIdType.MESH
GX = ("z", "a")
GY = ("y", "b", "c")
B = 128
CH = 2
RH = 4
EARLY = (0, -1, 1, -2, 2)
LATE = (-3, 3, 4)
PAD = 8
KP = 32
N = 16

A0, A1, A2, A3, A4 = 2.25, -2.4375, 1.6875, -0.5625, 0.0625


def split(x):
    hi = x.astype(jnp.bfloat16)
    lo = (x - hi.astype(jnp.float32)).astype(jnp.bfloat16)
    return hi, lo


def fold4(full):
    return (full[:B, :B] + full[B:, :B]) + (full[:B, B:] + full[B:, B:])


def kernel(
    g_hbm, a_hbm, both_out,
    a_in, gt, GI, GJ, R1, C1, R2, C2, CB, held, a_new, s_new, r_own, r_new,
    in_sem, gi_sem, gj_sem, gs_sem, down_sem, swap_sem, piece_sem, send_sem, *gather_sems,
):
    z, a = lax.axis_index("z"), lax.axis_index("a")
    y, b, c = lax.axis_index("y"), lax.axis_index("b"), lax.axis_index("c")
    a1, b1, c1 = 1 - a, 1 - b, 1 - c
    x = 2 * b + a
    gi = z * 2 + c
    gj = y * 4 + x
    own = c * 8 + y * 2 + b
    home = z == 2 * y + b
    swaps = a != c

    sems1, sems2 = gather_sems[:7], gather_sems[7:]
    s_out, r_out = both_out.at[0], both_out.at[1]
    load_g = pltpu.make_async_copy(g_hbm, gt, in_sem.at[0])
    load_a = pltpu.make_async_copy(a_hbm, a_in, in_sem.at[1])
    load_g.start()
    load_a.start()

    barrier = pltpu.get_barrier_semaphore()

    def greet(**where):
        pl.semaphore_signal(barrier, inc=1, device_id=where, device_id_type=MESH)

    def zs(dz):
        return lax.rem(z + dz + 8, 8)

    def ys(dy):
        return lax.rem(y + dy + 4, 4)

    def xs(dx):
        to = lax.rem(x + dx + 4, 4)
        return {"b": to // 2, "a": lax.rem(to, 2)}

    others = [
        {"y": ys(dy), "b": pb, "c": pc}
        for dy in (2, 1, -1, 0) for pb in (b1, b) for pc in (c1, c)
    ][:-1]

    @pl.when(c == 0)
    def _():
        for where in others:
            greet(z=2 * y + b, **where)

        @pl.when(jnp.logical_not(home))
        def _():
            greet(z=2 * y + b)

    for where in others:
        greet(a=c, **where)

    @pl.when(swaps)
    def _():
        greet(a=c)

    @pl.when(swaps)
    def _():
        greet(a=a1, c=c1)

    @pl.when(c == 1)
    def _():
        greet(c=0)

    for dz in (2, -2, 1, -1):
        greet(z=zs(dz))
    for d in (2, 1, -1):
        greet(y=ys(d))
        greet(**xs(d))
    greet(c=c1)
    alike = jnp.where(a == c, 1, 0)
    at_home = jnp.where(home, 1, 0)
    expected = 36 - 2 * alike + (1 - c) - (1 - c) * at_home

    load_g.wait()
    pl.semaphore_wait(barrier, expected)

    sends = []

    def start(src, dst, ssem, rsem, **where):
        copy = pltpu.make_async_remote_copy(
            src_ref=src, dst_ref=dst, send_sem=ssem, recv_sem=rsem,
            device_id=where, device_id_type=MESH,
        )
        copy.start()

    def send(src, dst, rsem, cond, **where):
        copy = pltpu.make_async_remote_copy(
            src_ref=src, dst_ref=dst, send_sem=send_sem.at[len(sends)], recv_sem=rsem,
            device_id=where, device_id_type=MESH,
        )
        pl.when(cond)(copy.start)
        sends.append((copy, cond))

    def left_here(ref, ssem):
        pltpu.make_async_remote_copy(
            src_ref=ref, dst_ref=ref, send_sem=ssem, recv_sem=gs_sem,
            device_id={"c": c1}, device_id_type=MESH,
        ).wait_send()

    def arrived(ref, rsem):
        pltpu.make_async_remote_copy(
            src_ref=ref, dst_ref=ref, send_sem=gs_sem, recv_sem=rsem,
            device_id={"c": c1}, device_id_type=MESH,
        ).wait_recv()

    col_y, col_b = z // 2, lax.rem(z, 2)
    for dz in (4, 3, 5, 2, 6, 1, 7):
        start(gt, GJ.at[own], piece_sem, gj_sem.at[c], z=zs(dz), y=col_y, b=col_b, c=0)
    away = jnp.logical_not(jnp.logical_and(home, c == 0))
    send(gt, GJ.at[own], gj_sem.at[c], away, y=col_y, b=col_b, c=0)
    for dx in (2, 1, -1, 0):
        for dy in (2, 1, -1, 0):
            if dx or dy:
                to = xs(dx)
                start(gt, GI.at[own], piece_sem, gi_sem, y=ys(dy), b=to["b"], a=to["a"], c=a)
    send(gt, GI.at[own], gi_sem, swaps, c=a)

    load_a.wait()
    send(a_in, a_new, swap_sem.at[0], swaps, a=a1, c=c1)

    @pl.when(a == c)
    def _():
        GI[own] = gt[...]
        a_new[...] = a_in[...]

    @pl.when(jnp.logical_and(home, c == 0))
    def _():
        GJ[own] = gt[...]

    lower = GJ.at[pl.ds(0, 8)]
    upper = GJ.at[pl.ds(8, 8)]

    @pl.when(c == 0)
    def _():
        @pl.when(home)
        def _():
            arrived(GJ.at[pl.ds(0, 7)], gj_sem.at[0])

        @pl.when(jnp.logical_not(home))
        def _():
            arrived(lower, gj_sem.at[0])

    send(lower, lower, down_sem.at[0], c == 0, c=c1)

    @pl.when(a == c)
    def _():
        arrived(GI.at[pl.ds(0, N - 1)], gi_sem)

    @pl.when(swaps)
    def _():
        arrived(GI, gi_sem)
        arrived(a_new, swap_sem.at[0])

    def outer(part):
        left = jnp.transpose(GI[8 * part : 8 * part + 8].reshape(8 * KP, B))
        right = GJ[8 * part : 8 * part + 8].reshape(8 * KP, B)
        return fold4(jnp.dot(
            jnp.concatenate(split(left), axis=0), jnp.concatenate(split(right), axis=1),
            preferred_element_type=jnp.float32,
        ))

    @pl.when(c == 1)
    def _():
        arrived(lower, down_sem.at[0])

    held[0] = outer(0)

    @pl.when(c == 0)
    def _():
        arrived(upper, gj_sem.at[1])

    send(upper, upper, down_sem.at[1], c == 0, c=c1)

    @pl.when(c == 1)
    def _():
        arrived(upper, down_sem.at[1])

    stat = 0.9 * a_new[...] + (held[0] + outer(1)) / float(N * KP)
    R1[gj] = stat
    C1[gi] = stat

    def exchange(R, C, sems, rows, extra, ready):
        width = B // CH
        parts = [(h * width, width) for h in range(CH)]
        parts[-1] = (B - width, width + rows - B)
        chunks = range(CH)
        tall = B // RH
        pairs = [(h, h + RH // 2) for h in range(RH // 2)]
        leg_sem, rest_sem, far_sem, block_sem, twin_sem, row_sent, col_sent = sems

        def row_ref(dy, dx, h):
            k = ys(dy) * 4 + lax.rem(x + dx + 4, 4)
            return R.at[k, pl.ds(h * tall, tall)]

        def leg_of(d, h):
            return leg_sem.at[d % 4 - 1, h]

        def col_ref(dz, h):
            return C.at[zs(dz) * 2 + c, pl.ds(*parts[h])]

        def far_of(dz, h):
            return far_sem.at[0 if dz > 0 else 1, h]

        def block_of(dz):
            return block_sem.at[(1, -1, 3, -3, 4).index(dz)]

        def leg(ref, sem, **where):
            start(ref, ref, row_sent, sem, **where)

        def hop(ref, sem, **where):
            start(ref, ref, col_sent, sem, **where)

        def twin(ref, dz):
            hop(ref, twin_sem.at[0 if dz in EARLY else 1], c=c1)

        for h in chunks:
            for dz in (2, -2):
                hop(col_ref(0, h), far_of(-dz, h), z=zs(dz))
        for h in chunks:
            for dz in (1, -1):
                hop(col_ref(0, h), block_of(-dz), z=zs(dz))
        for h, v in pairs:
            for d in (2, 1, -1):
                leg(row_ref(0, 0, h), leg_of(-d, h), **xs(d))
                leg(row_ref(0, 0, v), leg_of(-d, v), y=ys(d))
        twin(C.at[gi], 0)
        for h, v in pairs:
            for d in (2, 1, -1):
                leg(row_ref(0, 0, v), rest_sem, **xs(d))
                leg(row_ref(0, 0, h), rest_sem, y=ys(d))

        for step in chunks:
            h, v = pairs[step]
            for d in (1, -1, 2):
                item = row_ref(0, d, h)
                arrived(item, leg_of(d, h))
                for e in (2, 1, -1):
                    leg(item, rest_sem, y=ys(e))
                item = row_ref(d, 0, v)
                arrived(item, leg_of(d, v))
                for e in (2, 1, -1):
                    leg(item, rest_sem, **xs(e))
            for sign in (1, -1):
                item = col_ref(-2 * sign, step)
                arrived(item, far_of(-2 * sign, step))
                if (step % 2 == 0) == (sign > 0):
                    hop(item, block_of(4), z=zs(2 * sign))
                hop(item, block_of(-3 * sign), z=zs(sign))
                twin(item, -2)
        for dz in (-1, 1) + LATE:
            item = C.at[zs(dz) * 2 + c]
            arrived(item, block_of(dz))
            twin(item, dz)
        extra()
        arrived(R.at[pl.ds(0, 12)], rest_sem)
        arrived(C.at[pl.ds(0, len(EARLY))], twin_sem.at[0])
        ready(EARLY)
        arrived(C.at[pl.ds(0, len(LATE))], twin_sem.at[1])

    def sent(R, C, sems):
        left_here(R.at[pl.ds(0, N - 1)], sems[-2])
        left_here(C.at[pl.ds(0, N - 1)], sems[-1])

    def give_stat():
        send(R1.at[gj], s_new, swap_sem.at[1], swaps, a=a1, c=c1)

    def strips(R, k):
        return split(jnp.concatenate([R[2 * k], R[2 * k + 1]], axis=1))

    def columns(C, k):
        rows = jnp.concatenate([C[2 * k, :B], C[2 * k + 1, :B]], axis=0)
        return jnp.concatenate(split(rows), axis=1)

    total = []
    norms = []

    def square(steps):
        if not norms:
            norms.append(jnp.zeros((PAD, B), jnp.float32))
            for k in range(N):
                block = R1[k]
                norms[0] = norms[0] + jnp.sum((block * block).reshape(B // PAD, PAD, B), axis=0)
        for dz in steps:
            k = zs(dz)
            CB[k] = columns(C1, k)
            total.append(jnp.dot(
                jnp.concatenate(strips(R1, k), axis=0), CB[k], preferred_element_type=jnp.float32
            ))
        if steps == EARLY:
            held[0] = fold4(sum(total[1:], total[0]))

    exchange(R1, C1, sems1, B, give_stat, square)
    early = len(EARLY)
    square(LATE)
    mid = held[0] + fold4(sum(total[early + 1 :], total[early]))
    R2[gj] = mid
    C2[gi, :B] = mid
    C2[gi, B:] = norms[0]

    def keep_stat():
        @pl.when(swaps)
        def _():
            arrived(s_new, swap_sem.at[1])
            s_out[...] = s_new[...]

        @pl.when(a == c)
        def _():
            s_out[...] = R1[gj]

    half = B // 2
    wide = [[], []]

    def powers(steps, halves):
        for part in halves:
            for dz in steps:
                k = zs(dz)
                both = jnp.concatenate([CB[k], columns(C2, k)], axis=1)
                hi, lo = strips(R2, k)
                cut = slice(part * half, part * half + half)
                wide[part].append(jnp.dot(
                    jnp.concatenate([hi[cut], lo[cut]], axis=0), both, preferred_element_type=jnp.float32
                ))

    def fold2(full):
        return (full[:half, :B] + full[half:, :B]) + (full[:half, B:] + full[half:, B:])

    def first_powers(steps):
        powers(steps, (0, 1))
        for part in (0, 1):
            full = sum(wide[part][1:], wide[part][0])
            held[0, part * half : part * half + half] = fold2(full[:, : 2 * B])
            held[1, part * half : part * half + half] = fold2(full[:, 2 * B:])

    exchange(R2, C2, sems2, B + PAD, keep_stat, first_powers)

    squares = jnp.zeros((PAD, B), jnp.float32)
    for k in range(N):
        squares = squares + C2[k, B:]
    whole = jnp.sum(squares, keepdims=True)
    inv = 1.0 / (2.0 * jnp.sqrt(whole / float(N * B)))
    rows = lax.broadcasted_iota(jnp.int32, (half, B), 0) + gi * B
    cols = lax.broadcasted_iota(jnp.int32, (half, B), 1) + gj * B

    for part in (0, 1):
        powers(LATE, (part,))
        full = sum(wide[part][early + 1 :], wide[part][early])
        cut = pl.ds(part * half, half)
        cube = held[0, cut] + fold2(full[:, : 2 * B])
        quad = held[1, cut] + fold2(full[:, 2 * B:])
        eye = jnp.where(rows + part * half == cols, A0, 0.0)
        tail = A2 * R2[gj, cut] + inv * (A3 * cube + inv * (A4 * quad))
        r_own[cut] = eye + inv * (A1 * R1[gj, cut] + inv * tail)
        send(r_own.at[cut], r_new.at[cut], swap_sem.at[2 + part], swaps, a=a1, c=c1)

    @pl.when(swaps)
    def _():
        for part in (0, 1):
            cut = pl.ds(part * half, half)
            arrived(r_new.at[cut], swap_sem.at[2 + part])
            r_out[cut] = r_new[cut]

    @pl.when(a == c)
    def _():
        r_out[...] = r_own[...]

    left_here(R1.at[pl.ds(0, 11), pl.ds(0, 2 * KP)], piece_sem)
    sent(R1, C1, sems1)
    sent(R2, C2, sems2)
    for copy, cond in sends:
        pl.when(cond)(copy.wait_send)


def local(gradient, stat_old):
    f32 = jnp.float32
    dma = pltpu.SemaphoreType.DMA
    tile = pltpu.VMEM((B, B), f32)
    pieces = pltpu.VMEM((N, KP, B), f32)
    strip = pltpu.VMEM((N, B, B), f32)
    gather_sems = [dma((3, RH)), dma, dma((2, CH)), dma((5,)), dma((2,)), dma, dma]
    both = pl.pallas_call(
        kernel,
        out_shape=pltpu.VMEM((2, B, B), f32),
        in_specs=[pl.BlockSpec(memory_space=pl.ANY)] * 2,
        out_specs=pl.BlockSpec(memory_space=pltpu.VMEM),
        scratch_shapes=[
            tile, pltpu.VMEM((KP, B), f32), pieces, pieces,
            strip, strip, strip, pltpu.VMEM((N, B + PAD, B), f32),
            pltpu.VMEM((N // 2, 2 * B, 2 * B), jnp.bfloat16),
            pltpu.VMEM((2, B, B), f32),
            tile, tile, tile, tile,
            dma((2,)), dma, dma((2,)), dma, dma((2,)), dma((4,)), dma, dma((9,)),
            *gather_sems, *gather_sems,
        ],
        compiler_params=pltpu.CompilerParams(collective_id=0, has_side_effects=True),
    )(gradient.T, stat_old)
    return both[0], both[1]


def solution(mesh):
    torus = Mesh(mesh.devices.reshape(8, 2, 4, 2, 2), ("z", "a", "y", "b", "c"))
    return jax.shard_map(
        local, mesh=torus, in_specs=(P(GX, GY), P(GX, GY)),
        out_specs=(P(GX, GY), P(GX, GY)), check_vma=False,
    )
```

```python
import jax
import jax.numpy as jnp
from jax import lax
from jax.experimental import pallas as pl
from jax.experimental.pallas import tpu as pltpu
from jax.sharding import Mesh
from jax.sharding import PartitionSpec as P

MESH = pl.DeviceIdType.MESH
GX = ("z", "a")
GY = ("y", "b", "c")
B = 128
CH = 2
RH = 4
EARLY = (0, -1, 1, -2, 2)
LATE = (-3, 3, 4)
PAD = 8
KP = 32
N = 16

A0, A1, A2, A3, A4 = 2.25, -2.4375, 1.6875, -0.5625, 0.0625


def split(x):
    hi = x.astype(jnp.bfloat16)
    lo = (x - hi.astype(jnp.float32)).astype(jnp.bfloat16)
    return hi, lo


def fold4(full):
    return (full[:B, :B] + full[B:, :B]) + (full[:B, B:] + full[B:, B:])


def kernel(
    g_hbm, a_hbm, both_out,
    a_in, gt, GI, GJ, R1, C1, R2, C2, CB, held, a_new, s_new, r_own, r_new,
    in_sem, gi_sem, gj_sem, gs_sem, down_sem, swap_sem, piece_sem, send_sem, *gather_sems,
):
    z, a = lax.axis_index("z"), lax.axis_index("a")
    y, b, c = lax.axis_index("y"), lax.axis_index("b"), lax.axis_index("c")
    a1, b1, c1 = 1 - a, 1 - b, 1 - c
    x = 2 * b + a
    gi = z * 2 + c
    gj = y * 4 + x
    own = c * 8 + y * 2 + b
    home = z == 2 * y + b
    swaps = a != c

    sems1, sems2 = gather_sems[:7], gather_sems[7:]
    s_out, r_out = both_out.at[0], both_out.at[1]
    load_g = pltpu.make_async_copy(g_hbm, gt, in_sem.at[0])
    load_a = pltpu.make_async_copy(a_hbm, a_in, in_sem.at[1])
    load_g.start()
    load_a.start()

    barrier = pltpu.get_barrier_semaphore()

    def greet(**where):
        pl.semaphore_signal(barrier, inc=1, device_id=where, device_id_type=MESH)

    def zs(dz):
        return lax.rem(z + dz + 8, 8)

    def ys(dy):
        return lax.rem(y + dy + 4, 4)

    def xs(dx):
        to = lax.rem(x + dx + 4, 4)
        return {"b": to // 2, "a": lax.rem(to, 2)}

    others = [
        {"y": ys(dy), "b": pb, "c": pc}
        for dy in (2, 1, -1, 0) for pb in (b1, b) for pc in (c1, c)
    ][:-1]

    @pl.when(c == 0)
    def _():
        for where in others:
            greet(z=2 * y + b, **where)

        @pl.when(jnp.logical_not(home))
        def _():
            greet(z=2 * y + b)

    for where in others:
        greet(a=c, **where)

    @pl.when(swaps)
    def _():
        greet(a=c)

    @pl.when(swaps)
    def _():
        greet(a=a1, c=c1)

    @pl.when(c == 1)
    def _():
        greet(c=0)

    for dz in (2, -2, 1, -1):
        greet(z=zs(dz))
    for d in (2, 1, -1):
        greet(y=ys(d))
        greet(**xs(d))
    greet(c=c1)
    alike = jnp.where(a == c, 1, 0)
    at_home = jnp.where(home, 1, 0)
    expected = 36 - 2 * alike + (1 - c) - (1 - c) * at_home

    load_g.wait()
    pl.semaphore_wait(barrier, expected)

    sends = []

    def start(src, dst, ssem, rsem, **where):
        copy = pltpu.make_async_remote_copy(
            src_ref=src, dst_ref=dst, send_sem=ssem, recv_sem=rsem,
            device_id=where, device_id_type=MESH,
        )
        copy.start()

    def send(src, dst, rsem, cond, **where):
        copy = pltpu.make_async_remote_copy(
            src_ref=src, dst_ref=dst, send_sem=send_sem.at[len(sends)], recv_sem=rsem,
            device_id=where, device_id_type=MESH,
        )
        pl.when(cond)(copy.start)
        sends.append((copy, cond))

    def left_here(ref, ssem):
        pltpu.make_async_remote_copy(
            src_ref=ref, dst_ref=ref, send_sem=ssem, recv_sem=gs_sem,
            device_id={"c": c1}, device_id_type=MESH,
        ).wait_send()

    def arrived(ref, rsem):
        pltpu.make_async_remote_copy(
            src_ref=ref, dst_ref=ref, send_sem=gs_sem, recv_sem=rsem,
            device_id={"c": c1}, device_id_type=MESH,
        ).wait_recv()

    col_y, col_b = z // 2, lax.rem(z, 2)
    for dz in (4, 3, 5, 2, 6, 1, 7):
        start(gt, GJ.at[own], piece_sem, gj_sem.at[c], z=zs(dz), y=col_y, b=col_b, c=0)
    away = jnp.logical_not(jnp.logical_and(home, c == 0))
    send(gt, GJ.at[own], gj_sem.at[c], away, y=col_y, b=col_b, c=0)
    for dx in (2, 1, -1, 0):
        for dy in (2, 1, -1, 0):
            if dx or dy:
                to = xs(dx)
                start(gt, GI.at[own], piece_sem, gi_sem, y=ys(dy), b=to["b"], a=to["a"], c=a)
    send(gt, GI.at[own], gi_sem, swaps, c=a)

    load_a.wait()
    send(a_in, a_new, swap_sem.at[0], swaps, a=a1, c=c1)

    @pl.when(a == c)
    def _():
        GI[own] = gt[...]
        a_new[...] = a_in[...]

    @pl.when(jnp.logical_and(home, c == 0))
    def _():
        GJ[own] = gt[...]

    lower = GJ.at[pl.ds(0, 8)]
    upper = GJ.at[pl.ds(8, 8)]

    @pl.when(c == 0)
    def _():
        @pl.when(home)
        def _():
            arrived(GJ.at[pl.ds(0, 7)], gj_sem.at[0])

        @pl.when(jnp.logical_not(home))
        def _():
            arrived(lower, gj_sem.at[0])

    send(lower, lower, down_sem.at[0], c == 0, c=c1)

    @pl.when(a == c)
    def _():
        arrived(GI.at[pl.ds(0, N - 1)], gi_sem)

    @pl.when(swaps)
    def _():
        arrived(GI, gi_sem)
        arrived(a_new, swap_sem.at[0])

    def outer(part):
        left = jnp.transpose(GI[8 * part : 8 * part + 8].reshape(8 * KP, B))
        right = GJ[8 * part : 8 * part + 8].reshape(8 * KP, B)
        return fold4(jnp.dot(
            jnp.concatenate(split(left), axis=0), jnp.concatenate(split(right), axis=1),
            preferred_element_type=jnp.float32,
        ))

    @pl.when(c == 1)
    def _():
        arrived(lower, down_sem.at[0])

    held[0] = outer(0)

    @pl.when(c == 0)
    def _():
        arrived(upper, gj_sem.at[1])

    send(upper, upper, down_sem.at[1], c == 0, c=c1)

    @pl.when(c == 1)
    def _():
        arrived(upper, down_sem.at[1])

    stat = 0.9 * a_new[...] + (held[0] + outer(1)) / float(N * KP)
    R1[gj] = stat
    C1[gi] = stat

    def exchange(R, C, sems, rows, extra, ready):
        width = B // CH
        parts = [(h * width, width) for h in range(CH)]
        parts[-1] = (B - width, width + rows - B)
        chunks = range(CH)
        tall = B // RH
        pairs = [(h, h + RH // 2) for h in range(RH // 2)]
        leg_sem, rest_sem, far_sem, block_sem, twin_sem, row_sent, col_sent = sems

        def row_ref(dy, dx, h):
            k = ys(dy) * 4 + lax.rem(x + dx + 4, 4)
            return R.at[k, pl.ds(h * tall, tall)]

        def leg_of(d, h):
            return leg_sem.at[d % 4 - 1, h]

        def col_ref(dz, h):
            return C.at[zs(dz) * 2 + c, pl.ds(*parts[h])]

        def far_of(dz, h):
            return far_sem.at[0 if dz > 0 else 1, h]

        def block_of(dz):
            return block_sem.at[(1, -1, 3, -3, 4).index(dz)]

        def leg(ref, sem, **where):
            start(ref, ref, row_sent, sem, **where)

        def hop(ref, sem, **where):
            start(ref, ref, col_sent, sem, **where)

        def twin(ref, dz):
            hop(ref, twin_sem.at[0 if dz in EARLY else 1], c=c1)

        for h in chunks:
            for dz in (2, -2):
                hop(col_ref(0, h), far_of(-dz, h), z=zs(dz))
        for h in chunks:
            for dz in (1, -1):
                hop(col_ref(0, h), block_of(-dz), z=zs(dz))
        for h, v in pairs:
            for d in (2, 1, -1):
                leg(row_ref(0, 0, h), leg_of(-d, h), **xs(d))
                leg(row_ref(0, 0, v), leg_of(-d, v), y=ys(d))
        twin(C.at[gi], 0)
        for h, v in pairs:
            for d in (2, 1, -1):
                leg(row_ref(0, 0, v), rest_sem, **xs(d))
                leg(row_ref(0, 0, h), rest_sem, y=ys(d))

        for step in chunks:
            h, v = pairs[step]
            for d in (1, -1, 2):
                item = row_ref(0, d, h)
                arrived(item, leg_of(d, h))
                for e in (2, 1, -1):
                    leg(item, rest_sem, y=ys(e))
                item = row_ref(d, 0, v)
                arrived(item, leg_of(d, v))
                for e in (2, 1, -1):
                    leg(item, rest_sem, **xs(e))
            for sign in (1, -1):
                item = col_ref(-2 * sign, step)
                arrived(item, far_of(-2 * sign, step))
                if (step % 2 == 0) == (sign > 0):
                    hop(item, block_of(4), z=zs(2 * sign))
                hop(item, block_of(-3 * sign), z=zs(sign))
                twin(item, -2)
        for dz in (-1, 1) + LATE:
            item = C.at[zs(dz) * 2 + c]
            arrived(item, block_of(dz))
            twin(item, dz)
        extra()
        arrived(R.at[pl.ds(0, 12)], rest_sem)
        arrived(C.at[pl.ds(0, len(EARLY))], twin_sem.at[0])
        ready(EARLY)
        arrived(C.at[pl.ds(0, len(LATE))], twin_sem.at[1])

    def sent(R, C, sems):
        left_here(R.at[pl.ds(0, N - 1)], sems[-2])
        left_here(C.at[pl.ds(0, N - 1)], sems[-1])

    def give_stat():
        send(R1.at[gj], s_new, swap_sem.at[1], swaps, a=a1, c=c1)

    def strips(R, k):
        return split(jnp.concatenate([R[2 * k], R[2 * k + 1]], axis=1))

    def columns(C, k):
        rows = jnp.concatenate([C[2 * k, :B], C[2 * k + 1, :B]], axis=0)
        return jnp.concatenate(split(rows), axis=1)

    total = []
    norms = []

    def square(steps):
        if not norms:
            norms.append(jnp.zeros((PAD, B), jnp.float32))
            for k in range(N):
                block = R1[k]
                norms[0] = norms[0] + jnp.sum((block * block).reshape(B // PAD, PAD, B), axis=0)
        for dz in steps:
            k = zs(dz)
            CB[k] = columns(C1, k)
            total.append(jnp.dot(
                jnp.concatenate(strips(R1, k), axis=0), CB[k], preferred_element_type=jnp.float32
            ))
        if steps == EARLY:
            held[0] = fold4(sum(total[1:], total[0]))

    exchange(R1, C1, sems1, B, give_stat, square)
    early = len(EARLY)
    square(LATE)
    mid = held[0] + fold4(sum(total[early + 1 :], total[early]))
    R2[gj] = mid
    C2[gi, :B] = mid
    C2[gi, B:] = norms[0]

    drained = []

    def keep_stat():
        @pl.when(swaps)
        def _():
            arrived(s_new, swap_sem.at[1])
            s_out[...] = s_new[...]

        @pl.when(a == c)
        def _():
            s_out[...] = R1[gj]

        left_here(R1.at[pl.ds(0, 11), pl.ds(0, 2 * KP)], piece_sem)
        sent(R1, C1, sems1)
        for copy, cond in sends:
            pl.when(cond)(copy.wait_send)
        drained.append(len(sends))

    half = B // 2
    wide = [[], []]

    def powers(steps, halves):
        for part in halves:
            for dz in steps:
                k = zs(dz)
                both = jnp.concatenate([CB[k], columns(C2, k)], axis=1)
                hi, lo = strips(R2, k)
                cut = slice(part * half, part * half + half)
                wide[part].append(jnp.dot(
                    jnp.concatenate([hi[cut], lo[cut]], axis=0), both, preferred_element_type=jnp.float32
                ))

    def fold2(full):
        return (full[:half, :B] + full[half:, :B]) + (full[:half, B:] + full[half:, B:])

    def first_powers(steps):
        powers(steps, (0, 1))
        for part in (0, 1):
            full = sum(wide[part][1:], wide[part][0])
            held[0, part * half : part * half + half] = fold2(full[:, : 2 * B])
            held[1, part * half : part * half + half] = fold2(full[:, 2 * B:])

    exchange(R2, C2, sems2, B + PAD, keep_stat, first_powers)

    squares = jnp.zeros((PAD, B), jnp.float32)
    for k in range(N):
        squares = squares + C2[k, B:]
    whole = jnp.sum(squares, keepdims=True)
    inv = 1.0 / (2.0 * jnp.sqrt(whole / float(N * B)))
    rows = lax.broadcasted_iota(jnp.int32, (half, B), 0) + gi * B
    cols = lax.broadcasted_iota(jnp.int32, (half, B), 1) + gj * B

    for part in (0, 1):
        powers(LATE, (part,))
        full = sum(wide[part][early + 1 :], wide[part][early])
        cut = pl.ds(part * half, half)
        cube = held[0, cut] + fold2(full[:, : 2 * B])
        quad = held[1, cut] + fold2(full[:, 2 * B:])
        eye = jnp.where(rows + part * half == cols, A0, 0.0)
        tail = A2 * R2[gj, cut] + inv * (A3 * cube + inv * (A4 * quad))
        r_own[cut] = eye + inv * (A1 * R1[gj, cut] + inv * tail)
        send(r_own.at[cut], r_new.at[cut], swap_sem.at[2 + part], swaps, a=a1, c=c1)

    sent(R2, C2, sems2)

    @pl.when(swaps)
    def _():
        for part in (0, 1):
            cut = pl.ds(part * half, half)
            arrived(r_new.at[cut], swap_sem.at[2 + part])
            r_out[cut] = r_new[cut]

    @pl.when(a == c)
    def _():
        r_out[...] = r_own[...]

    for copy, cond in sends[drained[0]:]:
        pl.when(cond)(copy.wait_send)


def local(gradient, stat_old):
    f32 = jnp.float32
    dma = pltpu.SemaphoreType.DMA
    tile = pltpu.VMEM((B, B), f32)
    pieces = pltpu.VMEM((N, KP, B), f32)
    strip = pltpu.VMEM((N, B, B), f32)
    gather_sems = [dma((3, RH)), dma, dma((2, CH)), dma((5,)), dma((2,)), dma, dma]
    both = pl.pallas_call(
        kernel,
        out_shape=pltpu.VMEM((2, B, B), f32),
        in_specs=[pl.BlockSpec(memory_space=pl.ANY)] * 2,
        out_specs=pl.BlockSpec(memory_space=pltpu.VMEM),
        scratch_shapes=[
            tile, pltpu.VMEM((KP, B), f32), pieces, pieces,
            strip, strip, strip, pltpu.VMEM((N, B + PAD, B), f32),
            pltpu.VMEM((N // 2, 2 * B, 2 * B), jnp.bfloat16),
            pltpu.VMEM((2, B, B), f32),
            tile, tile, tile, tile,
            dma((2,)), dma, dma((2,)), dma, dma((2,)), dma((4,)), dma, dma((9,)),
            *gather_sems, *gather_sems,
        ],
        compiler_params=pltpu.CompilerParams(collective_id=0, has_side_effects=True),
    )(gradient.T, stat_old)
    return both[0], both[1]


def solution(mesh):
    torus = Mesh(mesh.devices.reshape(8, 2, 4, 2, 2), ("z", "a", "y", "b", "c"))
    return jax.shard_map(
        local, mesh=torus, in_specs=(P(GX, GY), P(GX, GY)),
        out_specs=(P(GX, GY), P(GX, GY)), check_vma=False,
    )
```

```python
import jax
import jax.numpy as jnp
from jax import lax
from jax.experimental import pallas as pl
from jax.experimental.pallas import tpu as pltpu
from jax.sharding import Mesh
from jax.sharding import PartitionSpec as P

MESH = pl.DeviceIdType.MESH
GX = ("z", "a")
GY = ("y", "b", "c")
B = 128
CH = 2
RH = 4
EARLY = (0, -1, 1, -2, 2)
LATE = (-3, 3, 4)
PAD = 8
KP = 32
N = 16

A0, A1, A2, A3, A4 = 2.25, -2.4375, 1.6875, -0.5625, 0.0625


def split(x):
    hi = x.astype(jnp.bfloat16)
    lo = (x - hi.astype(jnp.float32)).astype(jnp.bfloat16)
    return hi, lo


def fold4(full):
    return (full[:B, :B] + full[B:, :B]) + (full[:B, B:] + full[B:, B:])


def kernel(
    g_hbm, a_hbm, both_out,
    a_in, gt, GI, GJ, R1, C1, R2, C2, CB, held, a_new, s_new, r_own, r_new,
    in_sem, gi_sem, gj_sem, gs_sem, down_sem, swap_sem, piece_sem, send_sem, *gather_sems,
):
    z, a = lax.axis_index("z"), lax.axis_index("a")
    y, b, c = lax.axis_index("y"), lax.axis_index("b"), lax.axis_index("c")
    a1, b1, c1 = 1 - a, 1 - b, 1 - c
    x = 2 * b + a
    gi = z * 2 + c
    gj = y * 4 + x
    own = c * 8 + y * 2 + b
    home = z == 2 * y + b
    swaps = a != c

    sems1, sems2 = gather_sems[:7], gather_sems[7:]
    s_out, r_out = both_out.at[0], both_out.at[1]
    load_g = pltpu.make_async_copy(g_hbm, gt, in_sem.at[0])
    load_a = pltpu.make_async_copy(a_hbm, a_in, in_sem.at[1])
    load_g.start()
    load_a.start()

    barrier = pltpu.get_barrier_semaphore()

    def greet(**where):
        pl.semaphore_signal(barrier, inc=1, device_id=where, device_id_type=MESH)

    def zs(dz):
        return lax.rem(z + dz + 8, 8)

    def ys(dy):
        return lax.rem(y + dy + 4, 4)

    def xs(dx):
        to = lax.rem(x + dx + 4, 4)
        return {"b": to // 2, "a": lax.rem(to, 2)}

    others = [
        {"y": ys(dy), "b": pb, "c": pc}
        for dy in (2, 1, -1, 0) for pb in (b1, b) for pc in (c1, c)
    ][:-1]

    @pl.when(c == 0)
    def _():
        for where in others:
            greet(z=2 * y + b, **where)

        @pl.when(jnp.logical_not(home))
        def _():
            greet(z=2 * y + b)

    for where in others:
        greet(a=c, **where)

    @pl.when(swaps)
    def _():
        greet(a=c)

    @pl.when(swaps)
    def _():
        greet(a=a1, c=c1)

    @pl.when(c == 1)
    def _():
        greet(c=0)

    for dz in (2, -2, 1, -1):
        greet(z=zs(dz))
    for d in (2, 1, -1):
        greet(y=ys(d))
        greet(**xs(d))
    greet(c=c1)
    alike = jnp.where(a == c, 1, 0)
    at_home = jnp.where(home, 1, 0)
    expected = 36 - 2 * alike + (1 - c) - (1 - c) * at_home

    load_g.wait()
    pl.semaphore_wait(barrier, expected)

    sends = []

    def start(src, dst, ssem, rsem, **where):
        copy = pltpu.make_async_remote_copy(
            src_ref=src, dst_ref=dst, send_sem=ssem, recv_sem=rsem,
            device_id=where, device_id_type=MESH,
        )
        copy.start()

    def send(src, dst, rsem, cond, **where):
        copy = pltpu.make_async_remote_copy(
            src_ref=src, dst_ref=dst, send_sem=send_sem.at[len(sends)], recv_sem=rsem,
            device_id=where, device_id_type=MESH,
        )
        pl.when(cond)(copy.start)
        sends.append((copy, cond))

    def left_here(ref, ssem):
        pltpu.make_async_remote_copy(
            src_ref=ref, dst_ref=ref, send_sem=ssem, recv_sem=gs_sem,
            device_id={"c": c1}, device_id_type=MESH,
        ).wait_send()

    def arrived(ref, rsem):
        pltpu.make_async_remote_copy(
            src_ref=ref, dst_ref=ref, send_sem=gs_sem, recv_sem=rsem,
            device_id={"c": c1}, device_id_type=MESH,
        ).wait_recv()

    col_y, col_b = z // 2, lax.rem(z, 2)
    for dz in (4, 3, 5, 2, 6, 1, 7):
        start(gt, GJ.at[own], piece_sem, gj_sem.at[c], z=zs(dz), y=col_y, b=col_b, c=0)
    away = jnp.logical_not(jnp.logical_and(home, c == 0))
    send(gt, GJ.at[own], gj_sem.at[c], away, y=col_y, b=col_b, c=0)
    for dx in (2, 1, -1, 0):
        for dy in (2, 1, -1, 0):
            if dx or dy:
                to = xs(dx)
                start(gt, GI.at[own], piece_sem, gi_sem, y=ys(dy), b=to["b"], a=to["a"], c=a)
    send(gt, GI.at[own], gi_sem, swaps, c=a)

    load_a.wait()
    send(a_in, a_new, swap_sem.at[0], swaps, a=a1, c=c1)

    @pl.when(a == c)
    def _():
        GI[own] = gt[...]
        a_new[...] = a_in[...]

    @pl.when(jnp.logical_and(home, c == 0))
    def _():
        GJ[own] = gt[...]

    lower = GJ.at[pl.ds(0, 8)]
    upper = GJ.at[pl.ds(8, 8)]

    @pl.when(c == 0)
    def _():
        @pl.when(home)
        def _():
            arrived(GJ.at[pl.ds(0, 7)], gj_sem.at[0])

        @pl.when(jnp.logical_not(home))
        def _():
            arrived(lower, gj_sem.at[0])

    send(lower, lower, down_sem.at[0], c == 0, c=c1)

    @pl.when(a == c)
    def _():
        arrived(GI.at[pl.ds(0, N - 1)], gi_sem)

    @pl.when(swaps)
    def _():
        arrived(GI, gi_sem)
        arrived(a_new, swap_sem.at[0])

    def outer(part):
        left = jnp.transpose(GI[8 * part : 8 * part + 8].reshape(8 * KP, B))
        right = GJ[8 * part : 8 * part + 8].reshape(8 * KP, B)
        return fold4(jnp.dot(
            jnp.concatenate(split(left), axis=0), jnp.concatenate(split(right), axis=1),
            preferred_element_type=jnp.float32,
        ))

    @pl.when(c == 1)
    def _():
        arrived(lower, down_sem.at[0])

    held[0] = outer(0)

    @pl.when(c == 0)
    def _():
        arrived(upper, gj_sem.at[1])

    send(upper, upper, down_sem.at[1], c == 0, c=c1)

    @pl.when(c == 1)
    def _():
        arrived(upper, down_sem.at[1])

    stat = 0.9 * a_new[...] + (held[0] + outer(1)) / float(N * KP)
    R1[gj] = stat
    C1[gi] = stat

    def exchange(R, C, sems, rows, extra, ready):
        width = B // CH
        parts = [(h * width, width) for h in range(CH)]
        parts[-1] = (B - width, width + rows - B)
        chunks = range(CH)
        tall = B // RH
        pairs = [(h, h + RH // 2) for h in range(RH // 2)]
        leg_sem, rest_sem, far_sem, block_sem, twin_sem, row_sent, col_sent = sems

        def row_ref(dy, dx, h):
            k = ys(dy) * 4 + lax.rem(x + dx + 4, 4)
            return R.at[k, pl.ds(h * tall, tall)]

        def leg_of(d, h):
            return leg_sem.at[d % 4 - 1, h]

        def col_ref(dz, h):
            return C.at[zs(dz) * 2 + c, pl.ds(*parts[h])]

        def far_of(dz, h):
            return far_sem.at[0 if dz > 0 else 1, h]

        def block_of(dz):
            return block_sem.at[(1, -1, 3, -3, 4).index(dz)]

        def leg(ref, sem, **where):
            start(ref, ref, row_sent, sem, **where)

        def hop(ref, sem, **where):
            start(ref, ref, col_sent, sem, **where)

        def twin(ref, dz):
            hop(ref, twin_sem.at[0 if dz in EARLY else 1], c=c1)

        for h in chunks:
            for dz in (2, -2):
                hop(col_ref(0, h), far_of(-dz, h), z=zs(dz))
        for h in chunks:
            for dz in (1, -1):
                hop(col_ref(0, h), block_of(-dz), z=zs(dz))
        for h, v in pairs:
            for d in (2, 1, -1):
                leg(row_ref(0, 0, h), leg_of(-d, h), **xs(d))
                leg(row_ref(0, 0, v), leg_of(-d, v), y=ys(d))
        twin(C.at[gi], 0)
        for h, v in pairs:
            for d in (2, 1, -1):
                leg(row_ref(0, 0, v), rest_sem, **xs(d))
                leg(row_ref(0, 0, h), rest_sem, y=ys(d))

        for step in chunks:
            h, v = pairs[step]
            for d in (1, -1):
                item = row_ref(0, d, h)
                arrived(item, leg_of(d, h))
                for e in (2, 1, -1):
                    leg(item, rest_sem, y=ys(e))
                item = row_ref(d, 0, v)
                arrived(item, leg_of(d, v))
                for e in (2, 1, -1):
                    leg(item, rest_sem, **xs(e))
            for sign in (1, -1):
                item = col_ref(-2 * sign, step)
                arrived(item, far_of(-2 * sign, step))
                if (step % 2 == 0) == (sign > 0):
                    hop(item, block_of(4), z=zs(2 * sign))
                hop(item, block_of(-3 * sign), z=zs(sign))
                twin(item, -2)
            for d in (2,):
                item = row_ref(0, d, h)
                arrived(item, leg_of(d, h))
                for e in (2, 1, -1):
                    leg(item, rest_sem, y=ys(e))
                item = row_ref(d, 0, v)
                arrived(item, leg_of(d, v))
                for e in (2, 1, -1):
                    leg(item, rest_sem, **xs(e))
        for dz in (-1, 1) + LATE:
            item = C.at[zs(dz) * 2 + c]
            arrived(item, block_of(dz))
            twin(item, dz)
        arrived(R.at[pl.ds(0, 12)], rest_sem)
        extra()
        arrived(C.at[pl.ds(0, len(EARLY))], twin_sem.at[0])
        ready(EARLY)
        arrived(C.at[pl.ds(0, len(LATE))], twin_sem.at[1])

    def sent(R, C, sems):
        left_here(R.at[pl.ds(0, N - 1)], sems[-2])
        left_here(C.at[pl.ds(0, N - 1)], sems[-1])

    def give_stat():
        send(R1.at[gj], s_new, swap_sem.at[1], swaps, a=a1, c=c1)

    def strips(R, k):
        return split(jnp.concatenate([R[2 * k], R[2 * k + 1]], axis=1))

    def columns(C, k):
        rows = jnp.concatenate([C[2 * k, :B], C[2 * k + 1, :B]], axis=0)
        return jnp.concatenate(split(rows), axis=1)

    total = []
    norms = []

    def square(steps):
        if not norms:
            norms.append(jnp.zeros((PAD, B), jnp.float32))
            for k in range(N):
                block = R1[k]
                norms[0] = norms[0] + jnp.sum((block * block).reshape(B // PAD, PAD, B), axis=0)
        for dz in steps:
            k = zs(dz)
            CB[k] = columns(C1, k)
            total.append(jnp.dot(
                jnp.concatenate(strips(R1, k), axis=0), CB[k], preferred_element_type=jnp.float32
            ))
        if steps == EARLY:
            held[0] = fold4(sum(total[1:], total[0]))

    exchange(R1, C1, sems1, B, give_stat, square)
    early = len(EARLY)
    square(LATE)
    mid = held[0] + fold4(sum(total[early + 1 :], total[early]))
    R2[gj] = mid
    C2[gi, :B] = mid
    C2[gi, B:] = norms[0]

    def keep_stat():
        @pl.when(swaps)
        def _():
            arrived(s_new, swap_sem.at[1])
            s_out[...] = s_new[...]

        @pl.when(a == c)
        def _():
            s_out[...] = R1[gj]

    half = B // 2
    wide = [[], []]

    def powers(steps, halves):
        for part in halves:
            for dz in steps:
                k = zs(dz)
                both = jnp.concatenate([CB[k], columns(C2, k)], axis=1)
                hi, lo = strips(R2, k)
                cut = slice(part * half, part * half + half)
                wide[part].append(jnp.dot(
                    jnp.concatenate([hi[cut], lo[cut]], axis=0), both, preferred_element_type=jnp.float32
                ))

    def fold2(full):
        return (full[:half, :B] + full[half:, :B]) + (full[:half, B:] + full[half:, B:])

    def first_powers(steps):
        powers(steps, (0, 1))
        for part in (0, 1):
            full = sum(wide[part][1:], wide[part][0])
            held[0, part * half : part * half + half] = fold2(full[:, : 2 * B])
            held[1, part * half : part * half + half] = fold2(full[:, 2 * B:])

    exchange(R2, C2, sems2, B + PAD, keep_stat, first_powers)

    squares = jnp.zeros((PAD, B), jnp.float32)
    for k in range(N):
        squares = squares + C2[k, B:]
    whole = jnp.sum(squares, keepdims=True)
    inv = 1.0 / (2.0 * jnp.sqrt(whole / float(N * B)))
    rows = lax.broadcasted_iota(jnp.int32, (half, B), 0) + gi * B
    cols = lax.broadcasted_iota(jnp.int32, (half, B), 1) + gj * B

    for part in (0, 1):
        powers(LATE, (part,))
        full = sum(wide[part][early + 1 :], wide[part][early])
        cut = pl.ds(part * half, half)
        cube = held[0, cut] + fold2(full[:, : 2 * B])
        quad = held[1, cut] + fold2(full[:, 2 * B:])
        eye = jnp.where(rows + part * half == cols, A0, 0.0)
        tail = A2 * R2[gj, cut] + inv * (A3 * cube + inv * (A4 * quad))
        r_own[cut] = eye + inv * (A1 * R1[gj, cut] + inv * tail)
        send(r_own.at[cut], r_new.at[cut], swap_sem.at[2 + part], swaps, a=a1, c=c1)

    @pl.when(swaps)
    def _():
        for part in (0, 1):
            cut = pl.ds(part * half, half)
            arrived(r_new.at[cut], swap_sem.at[2 + part])
            r_out[cut] = r_new[cut]

    @pl.when(a == c)
    def _():
        r_out[...] = r_own[...]

    left_here(R1.at[pl.ds(0, 11), pl.ds(0, 2 * KP)], piece_sem)
    sent(R1, C1, sems1)
    sent(R2, C2, sems2)
    for copy, cond in sends:
        pl.when(cond)(copy.wait_send)


def local(gradient, stat_old):
    f32 = jnp.float32
    dma = pltpu.SemaphoreType.DMA
    tile = pltpu.VMEM((B, B), f32)
    pieces = pltpu.VMEM((N, KP, B), f32)
    strip = pltpu.VMEM((N, B, B), f32)
    gather_sems = [dma((3, RH)), dma, dma((2, CH)), dma((5,)), dma((2,)), dma, dma]
    both = pl.pallas_call(
        kernel,
        out_shape=pltpu.VMEM((2, B, B), f32),
        in_specs=[pl.BlockSpec(memory_space=pl.ANY)] * 2,
        out_specs=pl.BlockSpec(memory_space=pltpu.VMEM),
        scratch_shapes=[
            tile, pltpu.VMEM((KP, B), f32), pieces, pieces,
            strip, strip, strip, pltpu.VMEM((N, B + PAD, B), f32),
            pltpu.VMEM((N // 2, 2 * B, 2 * B), jnp.bfloat16),
            pltpu.VMEM((2, B, B), f32),
            tile, tile, tile, tile,
            dma((2,)), dma, dma((2,)), dma, dma((2,)), dma((4,)), dma, dma((9,)),
            *gather_sems, *gather_sems,
        ],
        compiler_params=pltpu.CompilerParams(collective_id=0, has_side_effects=True),
    )(gradient.T, stat_old)
    return both[0], both[1]


def solution(mesh):
    torus = Mesh(mesh.devices.reshape(8, 2, 4, 2, 2), ("z", "a", "y", "b", "c"))
    return jax.shard_map(
        local, mesh=torus, in_specs=(P(GX, GY), P(GX, GY)),
        out_specs=(P(GX, GY), P(GX, GY)), check_vma=False,
    )
```

```python
import jax
import jax.numpy as jnp
from jax import lax
from jax.experimental import pallas as pl
from jax.experimental.pallas import tpu as pltpu
from jax.sharding import Mesh
from jax.sharding import PartitionSpec as P

MESH = pl.DeviceIdType.MESH
GX = ("z", "a")
GY = ("y", "b", "c")
B = 128
CH = 2
RH = 4
EARLY = (0, -1, 1, -2, 2)
LATE = (-3, 3, 4)
PAD = 8
KP = 32
N = 16

A0, A1, A2, A3, A4 = 2.25, -2.4375, 1.6875, -0.5625, 0.0625


def split(x):
    hi = x.astype(jnp.bfloat16)
    lo = (x - hi.astype(jnp.float32)).astype(jnp.bfloat16)
    return hi, lo


def fold4(full):
    return (full[:B, :B] + full[B:, :B]) + (full[:B, B:] + full[B:, B:])


def kernel(
    g_hbm, a_hbm, both_out,
    a_in, gt, GI, GJ, R1, C1, R2, C2, CB, held, a_new, s_new, r_own, r_new,
    in_sem, gi_sem, gj_sem, gs_sem, down_sem, swap_sem, piece_sem, send_sem, *gather_sems,
):
    z, a = lax.axis_index("z"), lax.axis_index("a")
    y, b, c = lax.axis_index("y"), lax.axis_index("b"), lax.axis_index("c")
    a1, b1, c1 = 1 - a, 1 - b, 1 - c
    x = 2 * b + a
    gi = z * 2 + c
    gj = y * 4 + x
    own = c * 8 + y * 2 + b
    home = z == 2 * y + b
    swaps = a != c

    sems1, sems2 = gather_sems[:7], gather_sems[7:]
    s_out, r_out = both_out.at[0], both_out.at[1]
    load_g = pltpu.make_async_copy(g_hbm, gt, in_sem.at[0])
    load_a = pltpu.make_async_copy(a_hbm, a_in, in_sem.at[1])
    load_g.start()
    load_a.start()

    barrier = pltpu.get_barrier_semaphore()

    def greet(**where):
        pl.semaphore_signal(barrier, inc=1, device_id=where, device_id_type=MESH)

    def zs(dz):
        return lax.rem(z + dz + 8, 8)

    def ys(dy):
        return lax.rem(y + dy + 4, 4)

    def xs(dx):
        to = lax.rem(x + dx + 4, 4)
        return {"b": to // 2, "a": lax.rem(to, 2)}

    others = [
        {"y": ys(dy), "b": pb, "c": pc}
        for dy in (2, 1, -1, 0) for pb in (b1, b) for pc in (c1, c)
    ][:-1]

    @pl.when(c == 0)
    def _():
        for where in others:
            greet(z=2 * y + b, **where)

        @pl.when(jnp.logical_not(home))
        def _():
            greet(z=2 * y + b)

    for where in others:
        greet(a=c, **where)

    @pl.when(swaps)
    def _():
        greet(a=c)

    @pl.when(swaps)
    def _():
        greet(a=a1, c=c1)

    @pl.when(c == 1)
    def _():
        greet(c=0)

    for dz in (2, -2, 1, -1):
        greet(z=zs(dz))
    for d in (2, 1, -1):
        greet(y=ys(d))
        greet(**xs(d))
    greet(c=c1)
    alike = jnp.where(a == c, 1, 0)
    at_home = jnp.where(home, 1, 0)
    expected = 36 - 2 * alike + (1 - c) - (1 - c) * at_home

    load_g.wait()
    pl.semaphore_wait(barrier, expected)

    sends = []

    def start(src, dst, ssem, rsem, **where):
        copy = pltpu.make_async_remote_copy(
            src_ref=src, dst_ref=dst, send_sem=ssem, recv_sem=rsem,
            device_id=where, device_id_type=MESH,
        )
        copy.start()

    def send(src, dst, rsem, cond, **where):
        copy = pltpu.make_async_remote_copy(
            src_ref=src, dst_ref=dst, send_sem=send_sem.at[len(sends)], recv_sem=rsem,
            device_id=where, device_id_type=MESH,
        )
        pl.when(cond)(copy.start)
        sends.append((copy, cond))

    def left_here(ref, ssem):
        pltpu.make_async_remote_copy(
            src_ref=ref, dst_ref=ref, send_sem=ssem, recv_sem=gs_sem,
            device_id={"c": c1}, device_id_type=MESH,
        ).wait_send()

    def arrived(ref, rsem):
        pltpu.make_async_remote_copy(
            src_ref=ref, dst_ref=ref, send_sem=gs_sem, recv_sem=rsem,
            device_id={"c": c1}, device_id_type=MESH,
        ).wait_recv()

    col_y, col_b = z // 2, lax.rem(z, 2)
    for dz in (4, 3, 5, 2, 6, 1, 7):
        start(gt, GJ.at[own], piece_sem, gj_sem.at[c], z=zs(dz), y=col_y, b=col_b, c=0)
    away = jnp.logical_not(jnp.logical_and(home, c == 0))
    send(gt, GJ.at[own], gj_sem.at[c], away, y=col_y, b=col_b, c=0)
    for dx in (2, 1, -1, 0):
        for dy in (2, 1, -1, 0):
            if dx or dy:
                to = xs(dx)
                start(gt, GI.at[own], piece_sem, gi_sem, y=ys(dy), b=to["b"], a=to["a"], c=a)
    send(gt, GI.at[own], gi_sem, swaps, c=a)

    load_a.wait()
    send(a_in, a_new, swap_sem.at[0], swaps, a=a1, c=c1)

    @pl.when(a == c)
    def _():
        GI[own] = gt[...]
        a_new[...] = a_in[...]

    @pl.when(jnp.logical_and(home, c == 0))
    def _():
        GJ[own] = gt[...]

    lower = GJ.at[pl.ds(0, 8)]
    upper = GJ.at[pl.ds(8, 8)]

    @pl.when(c == 0)
    def _():
        @pl.when(home)
        def _():
            arrived(GJ.at[pl.ds(0, 7)], gj_sem.at[0])

        @pl.when(jnp.logical_not(home))
        def _():
            arrived(lower, gj_sem.at[0])

    send(lower, lower, down_sem.at[0], c == 0, c=c1)

    @pl.when(a == c)
    def _():
        arrived(GI.at[pl.ds(0, N - 1)], gi_sem)

    @pl.when(swaps)
    def _():
        arrived(GI, gi_sem)
        arrived(a_new, swap_sem.at[0])

    def outer(part):
        left = jnp.transpose(GI[8 * part : 8 * part + 8].reshape(8 * KP, B))
        right = GJ[8 * part : 8 * part + 8].reshape(8 * KP, B)
        return fold4(jnp.dot(
            jnp.concatenate(split(left), axis=0), jnp.concatenate(split(right), axis=1),
            preferred_element_type=jnp.float32,
        ))

    @pl.when(c == 1)
    def _():
        arrived(lower, down_sem.at[0])

    held[0] = outer(0)

    @pl.when(c == 0)
    def _():
        arrived(upper, gj_sem.at[1])

    send(upper, upper, down_sem.at[1], c == 0, c=c1)

    @pl.when(c == 1)
    def _():
        arrived(upper, down_sem.at[1])

    stat = 0.9 * a_new[...] + (held[0] + outer(1)) / float(N * KP)
    R1[gj] = stat
    C1[gi] = stat

    def exchange(R, C, sems, rows, extra, ready):
        width = B // CH
        parts = [(h * width, width) for h in range(CH)]
        parts[-1] = (B - width, width + rows - B)
        chunks = range(CH)
        tall = B // RH
        pairs = [(h, h + RH // 2) for h in range(RH // 2)]
        leg_sem, rest_sem, far_sem, block_sem, twin_sem, row_sent, col_sent = sems

        def row_ref(dy, dx, h):
            k = ys(dy) * 4 + lax.rem(x + dx + 4, 4)
            return R.at[k, pl.ds(h * tall, tall)]

        def leg_of(d, h):
            return leg_sem.at[d % 4 - 1, h]

        def col_ref(dz, h):
            return C.at[zs(dz) * 2 + c, pl.ds(*parts[h])]

        def far_of(dz, h):
            return far_sem.at[0 if dz > 0 else 1, h]

        def block_of(dz):
            return block_sem.at[(1, -1, 3, -3, 4).index(dz)]

        def leg(ref, sem, **where):
            start(ref, ref, row_sent, sem, **where)

        def hop(ref, sem, **where):
            start(ref, ref, col_sent, sem, **where)

        def twin(ref, dz):
            hop(ref, twin_sem.at[0 if dz in EARLY else 1], c=c1)

        for h in chunks:
            for dz in (2, -2):
                hop(col_ref(0, h), far_of(-dz, h), z=zs(dz))
        for h in chunks:
            for dz in (1, -1):
                hop(col_ref(0, h), block_of(-dz), z=zs(dz))
        for h, v in pairs:
            for d in (2, 1, -1):
                leg(row_ref(0, 0, h), leg_of(-d, h), **xs(d))
                leg(row_ref(0, 0, v), leg_of(-d, v), y=ys(d))
        twin(C.at[gi], 0)
        for h, v in pairs:
            for d in (2, 1, -1):
                leg(row_ref(0, 0, v), rest_sem, **xs(d))
                leg(row_ref(0, 0, h), rest_sem, y=ys(d))

        for step in chunks:
            h, v = pairs[step]
            for d in (1, -1, 2):
                item = row_ref(0, d, h)
                arrived(item, leg_of(d, h))
                for e in (2, 1, -1):
                    leg(item, rest_sem, y=ys(e))
                item = row_ref(d, 0, v)
                arrived(item, leg_of(d, v))
                for e in (2, 1, -1):
                    leg(item, rest_sem, **xs(e))
            for sign in (1, -1):
                item = col_ref(-2 * sign, step)
                arrived(item, far_of(-2 * sign, step))
                if (step % 2 == 0) == (sign > 0):
                    hop(item, block_of(4), z=zs(2 * sign))
                hop(item, block_of(-3 * sign), z=zs(sign))
                twin(item, -2)
        for dz in (-1, 1) + LATE:
            item = C.at[zs(dz) * 2 + c]
            arrived(item, block_of(dz))
            twin(item, dz)
        extra()
        arrived(R.at[pl.ds(0, 12)], rest_sem)
        arrived(C.at[pl.ds(0, len(EARLY))], twin_sem.at[0])
        ready(EARLY)
        arrived(C.at[pl.ds(0, len(LATE))], twin_sem.at[1])

    def sent(R, C, sems):
        left_here(R.at[pl.ds(0, N - 1)], sems[-2])
        left_here(C.at[pl.ds(0, N - 1)], sems[-1])

    def give_stat():
        send(R1.at[gj], s_new, swap_sem.at[1], swaps, a=a1, c=c1)

    def strips(R, k):
        return split(jnp.concatenate([R[2 * k], R[2 * k + 1]], axis=1))

    def columns(C, k):
        rows = jnp.concatenate([C[2 * k, :B], C[2 * k + 1, :B]], axis=0)
        return jnp.concatenate(split(rows), axis=1)

    total = []
    norms = []

    def square(steps):
        if not norms:
            norms.append(jnp.zeros((PAD, B), jnp.float32))
            for k in range(N):
                block = R1[k]
                norms[0] = norms[0] + jnp.sum((block * block).reshape(B // PAD, PAD, B), axis=0)
        for dz in steps:
            k = zs(dz)
            CB[k] = columns(C1, k)
            total.append(jnp.dot(
                jnp.concatenate(strips(R1, k), axis=0), CB[k], preferred_element_type=jnp.float32
            ))
        if steps == EARLY:
            held[0] = fold4(sum(total[1:], total[0]))

    exchange(R1, C1, sems1, B, give_stat, square)
    early = len(EARLY)
    square(LATE)
    mid = held[0] + fold4(sum(total[early + 1 :], total[early]))
    R2[gj] = mid
    C2[gi, :B] = mid
    C2[gi, B:] = norms[0]

    def keep_stat():
        @pl.when(swaps)
        def _():
            arrived(s_new, swap_sem.at[1])
            s_out[...] = s_new[...]

        @pl.when(a == c)
        def _():
            s_out[...] = R1[gj]

    spans = ((0, 96), (96, 32))
    wide = [[], []]

    def powers(steps, halves):
        for part in halves:
            for dz in steps:
                k = zs(dz)
                both = jnp.concatenate([CB[k], columns(C2, k)], axis=1)
                hi, lo = strips(R2, k)
                cut = slice(spans[part][0], sum(spans[part]))
                wide[part].append(jnp.dot(
                    jnp.concatenate([hi[cut], lo[cut]], axis=0), both, preferred_element_type=jnp.float32
                ))

    def fold2(full):
        half = full.shape[0] // 2
        return (full[:half, :B] + full[half:, :B]) + (full[:half, B:] + full[half:, B:])

    def first_powers(steps):
        powers(steps, (0, 1))
        for part in (0, 1):
            full = sum(wide[part][1:], wide[part][0])
            held[0, spans[part][0] : sum(spans[part])] = fold2(full[:, : 2 * B])
            held[1, spans[part][0] : sum(spans[part])] = fold2(full[:, 2 * B:])

    exchange(R2, C2, sems2, B + PAD, keep_stat, first_powers)

    squares = jnp.zeros((PAD, B), jnp.float32)
    for k in range(N):
        squares = squares + C2[k, B:]
    whole = jnp.sum(squares, keepdims=True)
    inv = 1.0 / (2.0 * jnp.sqrt(whole / float(N * B)))
    rows = lax.broadcasted_iota(jnp.int32, (B, B), 0) + gi * B
    cols = lax.broadcasted_iota(jnp.int32, (B, B), 1) + gj * B

    for part in (0, 1):
        powers(LATE, (part,))
        full = sum(wide[part][early + 1 :], wide[part][early])
        cut = pl.ds(*spans[part])
        cube = held[0, cut] + fold2(full[:, : 2 * B])
        quad = held[1, cut] + fold2(full[:, 2 * B:])
        eye = jnp.where(rows == cols, A0, 0.0)[spans[part][0] : sum(spans[part])]
        tail = A2 * R2[gj, cut] + inv * (A3 * cube + inv * (A4 * quad))
        r_own[cut] = eye + inv * (A1 * R1[gj, cut] + inv * tail)
        send(r_own.at[cut], r_new.at[cut], swap_sem.at[2 + part], swaps, a=a1, c=c1)

    @pl.when(swaps)
    def _():
        for part in (0, 1):
            cut = pl.ds(*spans[part])
            arrived(r_new.at[cut], swap_sem.at[2 + part])
            r_out[cut] = r_new[cut]

    @pl.when(a == c)
    def _():
        r_out[...] = r_own[...]

    left_here(R1.at[pl.ds(0, 11), pl.ds(0, 2 * KP)], piece_sem)
    sent(R1, C1, sems1)
    sent(R2, C2, sems2)
    for copy, cond in sends:
        pl.when(cond)(copy.wait_send)


def local(gradient, stat_old):
    f32 = jnp.float32
    dma = pltpu.SemaphoreType.DMA
    tile = pltpu.VMEM((B, B), f32)
    pieces = pltpu.VMEM((N, KP, B), f32)
    strip = pltpu.VMEM((N, B, B), f32)
    gather_sems = [dma((3, RH)), dma, dma((2, CH)), dma((5,)), dma((2,)), dma, dma]
    both = pl.pallas_call(
        kernel,
        out_shape=pltpu.VMEM((2, B, B), f32),
        in_specs=[pl.BlockSpec(memory_space=pl.ANY)] * 2,
        out_specs=pl.BlockSpec(memory_space=pltpu.VMEM),
        scratch_shapes=[
            tile, pltpu.VMEM((KP, B), f32), pieces, pieces,
            strip, strip, strip, pltpu.VMEM((N, B + PAD, B), f32),
            pltpu.VMEM((N // 2, 2 * B, 2 * B), jnp.bfloat16),
            pltpu.VMEM((2, B, B), f32),
            tile, tile, tile, tile,
            dma((2,)), dma, dma((2,)), dma, dma((2,)), dma((4,)), dma, dma((9,)),
            *gather_sems, *gather_sems,
        ],
        compiler_params=pltpu.CompilerParams(collective_id=0, has_side_effects=True),
    )(gradient.T, stat_old)
    return both[0], both[1]


def solution(mesh):
    torus = Mesh(mesh.devices.reshape(8, 2, 4, 2, 2), ("z", "a", "y", "b", "c"))
    return jax.shard_map(
        local, mesh=torus, in_specs=(P(GX, GY), P(GX, GY)),
        out_specs=(P(GX, GY), P(GX, GY)), check_vma=False,
    )
```
